256 devices in a mesh: dp: 8 (over z), ctx: 32 (over y, x, core).
Axes of the slice: x: 4, y: 4, z: 8, core: 2. Of those that a mesh axis runs over, the one named last changes fastest.
Arguments:
- queries: bfloat16 [65536, 2048], P(('dp', 'ctx')), parts along dimension 0, may hold values from -256 to 256
- key_rows: bfloat16 [65536, 2048], P(('dp', 'ctx')), parts along dimension 0, may hold values from -256 to 256
- values: bfloat16 [65536, 2048], P(('dp', 'ctx')), parts along dimension 0, may hold values from -6 to 6
- inner_rows: bfloat16 [65536, 4096], P(('dp', 'ctx')), parts along dimension 0, may hold values from -6 to 6
- conv_weight: float32 [4, 4096], replicated, may hold values from -3 to 3
- conv_bias: float32 [4096], replicated, may hold values from -3 to 3
- segment_ids: int32 [65536], P(('dp', 'ctx')), parts along dimension 0, may hold values from 0 to 3, never falling along the last dimension, each value on 1 to 4096 neighbouring positions
- block_reach: int32 [512], P(('dp', 'ctx')), parts along dimension 0, may hold values from 128 to 2048
- owner_counts: int32 [256], P('dp'), parts along dimension 0, may hold values from 1 to 3, as said below
Outputs:
- attn_owned: bfloat16 [98304, 2048], P(('dp', 'ctx')), parts along dimension 0
- conv_owned: bfloat16 [98304, 4096], P(('dp', 'ctx')), parts along dimension 0
The draws below stay inside these ranges and needn't reach their ends.
There are 8 independent parts, one for each index of `dp`. The reference program is written for one: setup_inputs(seed, part) draws one part's arguments, and reference() takes and returns one part's arrays. A program takes and returns all parts, laid end to end along the dimension named above; an argument that names none is the same for every part. Nothing has to cross between parts.
Inputs may be any that keep to these rules, and one draw needn't show every extreme that they name: `owner_counts`: the counts sum to 64. The blocks owned by the devices before device d number at least d * 2 and at most d * 2 + 1.
All inputs are finite; a program needn't handle non-finite values.
Results may differ from the reference program's by a relative error of at most 0.0047.
Values may be sent and summed in bfloat16 or wider, within the bound.
No kernel may reach another device: no remote copies, remote signals or barrier semaphores. Data moves between devices by JAX's collectives and lax.ppermute only.
A program may use at most 192 MiB of HBM per device.

```python
import math
import jax
import jax.numpy as jnp
import numpy as np
from jax import lax

HEADS = 16
D_HEAD = 128
CH = 4096
WINDOW = 2048
BLOCK = 128
KERNEL = 4
SEQ = 8192
FEAT = 2048
BPD = 2
MAXB = 3
NBLK = 64
DOCS = 4
DOC_MOST = 4096
N_CTX = 32


def attention_pair(key):
    key_draw = jax.random.normal(jax.random.fold_in(key, 101), (SEQ, FEAT), jnp.float32)
    query_draw = jax.random.normal(jax.random.fold_in(key, 102), (SEQ, FEAT), jnp.float32)
    return (query_draw, key_draw)


def draw_queries(key, part):
    return attention_pair(key)[0].astype(jnp.bfloat16)


def draw_key_rows(key, part):
    return attention_pair(key)[1].astype(jnp.bfloat16)


def draw_owner_counts(key, part):
    halfway = BPD // 2
    drift = jax.random.randint(jax.random.fold_in(key, 201), (N_CTX + 1,), 0, halfway + 1)
    widest = jax.random.randint(jax.random.fold_in(key, 202), (), 1, N_CTX - 1)
    places = jnp.arange(N_CTX + 1, dtype=jnp.int32)
    drift = jnp.where(places == widest, 0, drift)
    drift = jnp.where(places == widest + 1, halfway, drift)
    drift = jnp.where(places == widest + 2, 0, drift)
    drift = jnp.where((places == 0) | (places == N_CTX), 0, drift)
    return (BPD + drift[1:] - drift[:-1]).astype(jnp.int32)


def set_ends(values, stream_key, smallest, top_value):
    dims = values.shape
    index_at = [jax.random.randint(jax.random.fold_in(stream_key, axis), (), 0, dims[axis]) for axis in range(len(dims))]
    values = values.at[tuple(index_at)].set(smallest)
    longest = dims.index(max(dims))
    index_at[longest] = (index_at[longest] + 1) % dims[longest]
    return values.at[tuple(index_at)].set(top_value)


def shard_levels(key, dims, cuts, low, high):
    level, own = 1.0, jax.random.fold_in(key, 6)
    for position, blocks in cuts:
        steps = jnp.exp(jax.random.uniform(jax.random.fold_in(own, position), (blocks,), jnp.float32, low / len(cuts), high / len(cuts)))
        level = level * jnp.repeat(steps, dims[position] // blocks).reshape([-1 if axis == position else 1 for axis in range(len(dims))])
    return level


def length_profile(amount, total, reach, skew):
    weights = [(1 << 20) // math.isqrt(grade ** skew) + 1 for grade in range(2, amount + 1)]
    rest, holding = total - reach - (amount - 1), [1] * (amount - 1)
    while rest > 0:
        free = [i for i in range(amount - 1) if holding[i] < reach]
        whole, left = sum([weights[i] for i in free]), rest
        for i in free:
            addition = min(reach - holding[i], max(1, left * weights[i] // whole), rest)
            holding[i] = holding[i] + addition
            rest = rest - addition
    return np.array([reach] + holding)


def ragged(key, amount, total, bound, skew):
    if amount == 2:
        one = jax.random.randint(key, (), max(1, total - bound), min(bound, total - 1) + 1)
        return jnp.stack([one, total - one])
    lengths = jnp.asarray(length_profile(amount, total, bound, skew), jnp.int32)
    twos = (amount - 1) // 2
    donor, taker = lengths[1:1 + 2 * twos:2], lengths[2:2 + 2 * twos:2]
    slack = jnp.minimum(donor - 1, bound - taker)
    moved = jax.random.randint(jax.random.fold_in(key, 1), (twos,), 0, 1 << 20) % (slack + 1)
    lengths = lengths.at[1:1 + 2 * twos:2].set(donor - moved).at[2:2 + 2 * twos:2].set(taker + moved)
    return lengths[jax.random.permutation(jax.random.fold_in(key, 2), amount)]


def scatter_about(key, dims, deviation, reach, split=(), held_as=jnp.bfloat16):
    result = deviation * jax.random.normal(key, dims, jnp.float32)
    if split:
        result = result * shard_levels(key, dims, split, -0.22, 0.18)
    return jnp.clip(result, -reach, reach).astype(held_as)


def setup_inputs(seed: int = 0, part: int = 0) -> dict:
    key_of = jax.random.split(jax.random.key(seed), 10)
    part_keys = jax.random.split(jax.random.fold_in(key_of[9], part), 10)
    queries = draw_queries(jax.random.fold_in(jax.random.fold_in(key_of[9], part), 71), part)
    key_rows = draw_key_rows(jax.random.fold_in(jax.random.fold_in(key_of[9], part), 71), part)
    values = scatter_about(part_keys[2], (SEQ, FEAT), 1.0, 6.0, ((0, 32),))
    inner_rows = scatter_about(part_keys[3], (SEQ, CH), 1.0, 6.0, ((0, 32),))
    conv_weight = scatter_about(key_of[4], (KERNEL, CH), 0.5, 3.0, (), jnp.float32)
    conv_bias = scatter_about(key_of[5], (CH,), 0.5, 3.0, (), jnp.float32)
    segment_ids = jnp.searchsorted(jnp.cumsum(ragged(part_keys[6], DOCS, SEQ, DOC_MOST, 0)), jnp.arange(SEQ), side="right").astype(jnp.int32)
    block_reach = set_ends(jax.random.randint(part_keys[7], (NBLK,), BLOCK, WINDOW + 1), jax.random.fold_in(part_keys[7], 1), BLOCK, WINDOW).astype(jnp.int32)
    owner_counts = draw_owner_counts(jax.random.fold_in(jax.random.fold_in(key_of[9], part), 71), part)
    return dict(queries=queries, key_rows=key_rows, values=values, inner_rows=inner_rows, conv_weight=conv_weight, conv_bias=conv_bias, segment_ids=segment_ids, block_reach=block_reach, owner_counts=owner_counts)


masked_score = -1e+30

def attend(query_rows, key_span, value_span, query_seg, key_seg, block_first, reach_value):
    query_pos = block_first + jnp.arange(BLOCK, dtype=jnp.int32)
    key_pos = block_first - WINDOW + jnp.arange(WINDOW + BLOCK, dtype=jnp.int32)
    allowed = (key_pos[None, :] <= query_pos[:, None]) & (key_pos[None, :] > query_pos[:, None] - WINDOW)
    allowed = allowed & (key_pos[None, :] >= block_first - reach_value) & (key_pos[None, :] >= 0)
    allowed = allowed & (key_seg[None, :] == query_seg[:, None])
    heads_q = query_rows.reshape(BLOCK, HEADS, D_HEAD).astype(jnp.float32)
    heads_k = key_span.reshape(WINDOW + BLOCK, HEADS, D_HEAD).astype(jnp.float32)
    heads_v = value_span.reshape(WINDOW + BLOCK, HEADS, D_HEAD).astype(jnp.float32)
    scores = jnp.einsum('qhd,khd->hqk', heads_q, heads_k) * (1.0 / math.sqrt(D_HEAD))
    scores = jnp.where(allowed[None], scores, masked_score)
    row_top = lax.optimization_barrier(jnp.max(scores, axis=2, keepdims=True))
    lifted = jnp.where(allowed[None], jnp.exp(scores - row_top), 0.0)
    weights = (lifted / lax.optimization_barrier(jnp.sum(lifted, axis=2, keepdims=True))).astype(jnp.bfloat16)
    mixed = jnp.einsum('hqk,khd->qhd', weights.astype(jnp.float32), heads_v)
    return mixed.reshape(BLOCK, HEADS * D_HEAD).astype(jnp.bfloat16)

def convolve(ext_rows, ext_seg, ext_pos, conv_weight, conv_bias, row_count):
    lag = KERNEL - 1
    running = jnp.zeros((row_count, conv_bias.shape[0]), jnp.float32) + conv_bias[None, :]
    for offset in range(KERNEL):
        shifted = ext_rows[lag - offset:lag - offset + row_count].astype(jnp.float32)
        usable = (ext_seg[lag - offset:lag - offset + row_count] == ext_seg[lag:]) & (ext_pos[lag - offset:lag - offset + row_count] >= 0)
        running = running + conv_weight[offset][None, :] * jnp.where(usable[:, None], shifted, 0.0)
    return jax.nn.silu(running).astype(jnp.bfloat16)

def reference(queries, key_rows, values, inner_rows, conv_weight, conv_bias, segment_ids, block_reach, owner_counts):
    seq_len = queries.shape[0]
    features = queries.shape[1]
    lag = KERNEL - 1
    padded_keys = jnp.concatenate([jnp.zeros((WINDOW, features), key_rows.dtype), key_rows], axis=0)
    padded_values = jnp.concatenate([jnp.zeros((WINDOW, features), values.dtype), values], axis=0)
    padded_segs = jnp.concatenate([jnp.full((WINDOW,), -1, jnp.int32), segment_ids.astype(jnp.int32)], axis=0)

    def one_block(block_id):
        block_first = (block_id * BLOCK).astype(jnp.int32)
        query_part = lax.dynamic_slice_in_dim(queries, block_first, BLOCK, 0)
        query_segs = lax.dynamic_slice_in_dim(segment_ids.astype(jnp.int32), block_first, BLOCK, 0)
        key_part = lax.dynamic_slice_in_dim(padded_keys, block_first, WINDOW + BLOCK, 0)
        value_part = lax.dynamic_slice_in_dim(padded_values, block_first, WINDOW + BLOCK, 0)
        key_segs = lax.dynamic_slice_in_dim(padded_segs, block_first, WINDOW + BLOCK, 0)
        return attend(query_part, key_part, value_part, query_segs, key_segs, block_first, block_reach[block_id])
    attention = lax.map(one_block, jnp.arange(NBLK, dtype=jnp.int32)).reshape(seq_len, features)
    ext_rows = jnp.concatenate([jnp.zeros((lag, inner_rows.shape[1]), inner_rows.dtype), inner_rows], axis=0)
    ext_seg = jnp.concatenate([jnp.full((lag,), -1, jnp.int32), segment_ids.astype(jnp.int32)], axis=0)
    ext_pos = jnp.arange(seq_len + lag, dtype=jnp.int32) - lag
    mixed = convolve(ext_rows, ext_seg, ext_pos, conv_weight, conv_bias, seq_len)
    counts = owner_counts.astype(jnp.int32)
    first = (jnp.cumsum(counts) - counts).astype(jnp.int32)
    slot_rows = jnp.arange(MAXB * BLOCK, dtype=jnp.int32)
    token_index = first[:, None] * BLOCK + slot_rows[None, :]
    live = (slot_rows[None, :] < counts[:, None] * BLOCK).reshape(-1)
    token_index = jnp.clip(token_index, 0, seq_len - 1).reshape(-1).astype(jnp.int32)
    attn_owned = jnp.where(live[:, None], attention[token_index], 0).astype(attention.dtype)
    conv_owned = jnp.where(live[:, None], mixed[token_index], 0).astype(mixed.dtype)
    return (attn_owned, conv_owned)
```

```python
import functools
import math

import jax
import jax.numpy as jnp
from jax import lax
from jax.experimental import pallas as pl
from jax.experimental.pallas import tpu as pltpu
from jax.sharding import PartitionSpec as P

HEADS = 16
D_HEAD = 128
WINDOW = 2048
BLOCK = 128
HALF = BLOCK // 2
KERNEL = 4
N = 32
ROWS = 256
SLOTS = 3
MSG = 3 * BLOCK + 8
TILES = N // 2
WIDTHS = (4, 6, 8, 10)
EXP_SCALE = math.log2(math.e) / math.sqrt(D_HEAD)
MASKED = -1e30
GROUP = 4


def pack_kernel(reach_ref, seg_ref, q_ref, k_ref, v_ref, out_ref):
    seg = seg_ref[...]
    lane = lax.broadcasted_iota(jnp.int32, (8, 128), 1)
    meta = jnp.zeros((8, 128), jnp.int32)
    for v in range(3):
        count = jnp.sum((seg <= v).astype(jnp.int32))
        meta = jnp.where(lane == v, count, meta)
    for b in range(2):
        reach = reach_ref[b]
        meta = jnp.where(lane == 3 + 2 * b, reach // 16, meta)
        meta = jnp.where(lane == 4 + 2 * b, reach % 16, meta)
    meta = meta.astype(jnp.float32).astype(jnp.bfloat16)
    for h in range(GROUP):
        for c in range(2):
            for n, ref in enumerate((q_ref, k_ref, v_ref)):
                for b in range(2):
                    at = b * BLOCK + c * HALF
                    out_ref[2 * h + c, n * BLOCK + b * HALF : n * BLOCK + (b + 1) * HALF, :] = ref[
                        at : at + HALF, h * D_HEAD : (h + 1) * D_HEAD
                    ]
            out_ref[2 * h + c, 3 * BLOCK :, :] = meta


def pack(q, k, v, seg, reach):
    wide = pl.BlockSpec((ROWS, GROUP * D_HEAD), lambda g: (0, g))
    return pl.pallas_call(
        pack_kernel,
        grid=(HEADS // GROUP,),
        in_specs=[
            pl.BlockSpec(memory_space=pltpu.SMEM),
            pl.BlockSpec((2, 128), lambda g: (0, 0)),
            wide,
            wide,
            wide,
        ],
        out_specs=pl.BlockSpec((2 * GROUP, MSG, D_HEAD), lambda g: (g, 0, 0)),
        out_shape=jax.ShapeDtypeStruct((N, MSG, D_HEAD), jnp.bfloat16),
        name="pack",
    )(reach, seg.reshape(2, 128), q, k, v)


def attend_kernel(core_ref, counts_ref, mine_ref, theirs_ref, out_ref, bounds_ref, s_ref, slot_ref, kmin_ref):
    core = core_ref[0]

    def fill(e, first):
        count = counts_ref[e]
        for j in range(SLOTS):
            slot_ref[first + j] = SLOTS * e + j
        return first + count

    lax.fori_loop(0, N, fill, jnp.int32(0))
    out_ref[...] = jnp.zeros_like(out_ref)

    meta = mine_ref[:, 3 * BLOCK, :].astype(jnp.float32).astype(jnp.int32)
    totals = jnp.sum(meta, axis=0, keepdims=True)
    bounds = [totals[:, v : v + 1] for v in range(3)]
    lane1 = lax.broadcasted_iota(jnp.int32, (1, 128), 1)
    for v in range(3):
        bounds_ref[v] = jnp.sum(jnp.where(lane1 == v, totals, 0))

    def lowest(t, first, reach):
        lo = jnp.maximum(t - (WINDOW - 1), first - reach)
        lo = jnp.maximum(lo, 0)
        for bound in bounds:
            lo = jnp.maximum(lo, jnp.where(bound <= t, bound, 0))
        return lo

    source = lax.broadcasted_iota(jnp.int32, (N, 1), 0)
    reaches = [meta[:, 3 + 2 * b : 4 + 2 * b] * 16 + meta[:, 4 + 2 * b : 5 + 2 * b] for b in range(2)]
    firsts = [source * ROWS + b * BLOCK for b in range(2)]
    least = jnp.minimum(
        lowest(firsts[0], firsts[0], reaches[0]), lowest(firsts[1], firsts[1], reaches[1])
    )
    for i in range(TILES):
        kmin_ref[i] = jnp.min(jnp.where(source // 2 == i, least, 1 << 20))

    col = lax.broadcasted_iota(jnp.int32, (1, 256), 1)
    col = (
        (col % 128) // HALF * BLOCK
        + col % HALF
        + jnp.where(col < 128, core, 1 - core) * HALF
    )
    row = lax.broadcasted_iota(jnp.int32, (HALF, 1), 0) + core * HALF
    ones = jnp.ones((256, D_HEAD), jnp.bfloat16)

    def tile(i, width):
        q = jnp.concatenate([mine_ref[2 * i, :BLOCK, :], mine_ref[2 * i + 1, :BLOCK, :]], axis=0)
        times, lows = [], []
        for part in range(4):
            first = i * (2 * ROWS) + part * BLOCK
            t = first + row
            figures = mine_ref[2 * i + part // 2, 3 * BLOCK :, :].astype(jnp.float32).astype(jnp.int32)
            at = 3 + 2 * (part % 2)
            reach = figures[:1, at : at + 1] * 16 + figures[:1, at + 1 : at + 2]
            times.append(t)
            lows.append(lowest(t, first, reach))
        time = jnp.concatenate(times, axis=0)
        low = jnp.concatenate(lows, axis=0)
        start = 2 * i + 2 - width
        top = None
        for w in range(width):
            j = start + w
            held = jnp.maximum(j, 0)
            k = jnp.concatenate(
                [mine_ref[held, BLOCK : 2 * BLOCK, :], theirs_ref[held, BLOCK : 2 * BLOCK, :]], axis=0
            )
            s = lax.dot_general(q, k, (((1,), (1,)), ((), ())), preferred_element_type=jnp.float32)
            pos = col + j * ROWS
            allowed = pos >= low
            if w >= width - 2:
                allowed = allowed & (pos <= time)
            s = jnp.where(allowed, s, MASKED)
            s_ref[:, w * 256 : (w + 1) * 256] = s
            here = jnp.maximum(s[:, :128], s[:, 128:])
            top = here if top is None else jnp.maximum(top, here)
        top = jnp.max(top, axis=1, keepdims=True) * EXP_SCALE
        acc = None
        for w in range(width):
            held = jnp.maximum(start + w, 0)
            p = jnp.exp2(s_ref[:, w * 256 : (w + 1) * 256] * EXP_SCALE - top).astype(jnp.bfloat16)
            v = jnp.concatenate(
                [mine_ref[held, 2 * BLOCK : 3 * BLOCK, :], theirs_ref[held, 2 * BLOCK : 3 * BLOCK, :]], axis=0
            )
            v = jnp.concatenate([v, ones], axis=1)
            o = lax.dot_general(p, v, (((1,), (0,)), ((), ())), preferred_element_type=jnp.float32)
            acc = o if acc is None else acc + o
        o = (acc[:, :D_HEAD] / acc[:, D_HEAD:]).astype(jnp.bfloat16)
        for part in range(4):
            out_ref[slot_ref[4 * i + part]] = o[part * HALF : (part + 1) * HALF]

    def step(i, carry):
        need = 2 * i + 2 - kmin_ref[i] // ROWS
        below = 0
        for width in WIDTHS:
            @pl.when((need > below) & (need <= width))
            def _(width=width):
                tile(i, width)

            below = width
        return carry

    lax.fori_loop(0, TILES, step, 0)


def attention(mine, theirs, core, counts):
    smem = pl.BlockSpec(memory_space=pltpu.SMEM)
    vmem = pl.BlockSpec(memory_space=pltpu.VMEM)
    return pl.pallas_call(
        attend_kernel,
        in_specs=[smem, smem, vmem, vmem],
        out_specs=(vmem, smem),
        out_shape=(
            jax.ShapeDtypeStruct((N * SLOTS, HALF, D_HEAD), jnp.bfloat16),
            jax.ShapeDtypeStruct((4,), jnp.int32),
        ),
        scratch_shapes=[
            pltpu.VMEM((256, 256 * max(WIDTHS)), jnp.float32),
            pltpu.SMEM((2 * N + 8,), jnp.int32),
            pltpu.SMEM((TILES,), jnp.int32),
        ],
        cost_estimate=pl.CostEstimate(
            flops=10 * 10**9, bytes_accessed=8 * 2**20, transcendentals=10**7
        ),
        name="attend",
    )(core, counts, mine, theirs)


def gather_kernel(in_ref, out_ref):
    for h in range(HEADS):
        for c in range(2):
            out_ref[c * HALF : (c + 1) * HALF, h * D_HEAD : (h + 1) * D_HEAD] = in_ref[2 * h + c]


def assemble(received):
    return pl.pallas_call(
        gather_kernel,
        grid=(SLOTS,),
        in_specs=[pl.BlockSpec((N, HALF, D_HEAD), lambda j: (0, j, 0))],
        out_specs=pl.BlockSpec((BLOCK, HEADS * D_HEAD), lambda j: (j, 0)),
        out_shape=jax.ShapeDtypeStruct((SLOTS * BLOCK, HEADS * D_HEAD), jnp.bfloat16),
        name="assemble",
    )(received)


def conv_kernel(figures_ref, bounds_ref, inner_ref, next_ref, tail_ref, weight_ref, bias_ref, out_ref, ext_ref):
    index, off, count = figures_ref[0], figures_ref[1], figures_ref[2]
    ext_ref[:8, :] = tail_ref[...].astype(jnp.float32)
    ext_ref[8 : 8 + ROWS, :] = inner_ref[...].astype(jnp.float32)
    ext_ref[8 + ROWS :, :] = next_ref[...].astype(jnp.float32)
    for block in range(SLOTS):
        slot = block - off

        @pl.when((slot >= 0) & (slot < count))
        def _(block=block, slot=slot):
            time = index * ROWS + block * BLOCK + lax.broadcasted_iota(jnp.int32, (BLOCK, 1), 0)
            start = jnp.zeros_like(time)
            for v in range(3):
                start = jnp.maximum(start, jnp.where(bounds_ref[v] <= time, bounds_ref[v], 0))
            since = time - start
            at = 8 + block * BLOCK
            total = bias_ref[...] + weight_ref[0:1, :] * ext_ref[at : at + BLOCK, :]
            for j in range(1, KERNEL):
                row = jnp.where(since >= j, ext_ref[at - j : at - j + BLOCK, :], 0.0)
                total = total + weight_ref[j : j + 1, :] * row
            out_ref[pl.ds(pl.multiple_of(slot * BLOCK, BLOCK), BLOCK), :] = (
                total / (1.0 + jnp.exp(-total))
            ).astype(jnp.bfloat16)

    for slot in range(1, SLOTS):

        @pl.when(slot >= count)
        def _(slot=slot):
            out_ref[slot * BLOCK : (slot + 1) * BLOCK, :] = jnp.zeros((BLOCK, out_ref.shape[1]), jnp.bfloat16)


def convolve(figures, bounds, inner, following, tail, weight, bias):
    channels = inner.shape[1]
    width = 512
    smem = pl.BlockSpec(memory_space=pltpu.SMEM)

    def wide(rows):
        return pl.BlockSpec((rows, width), lambda g: (0, g))

    return pl.pallas_call(
        conv_kernel,
        grid=(channels // width,),
        in_specs=[smem, smem, wide(ROWS), wide(BLOCK), wide(8), wide(KERNEL), wide(1)],
        out_specs=wide(SLOTS * BLOCK),
        out_shape=jax.ShapeDtypeStruct((SLOTS * BLOCK, channels), jnp.bfloat16),
        scratch_shapes=[pltpu.VMEM((8 + ROWS + BLOCK, width), jnp.float32)],
        cost_estimate=pl.CostEstimate(
            flops=10 * 10**9, bytes_accessed=6 * 2**20, transcendentals=2 * 10**6
        ),
        name="conv",
    )(figures, bounds, inner, following, tail, weight, bias.reshape(1, -1))


def shards(queries, key_rows, values, inner_rows, conv_weight, conv_bias, segment_ids, block_reach, owner_counts):
    index = lax.axis_index("ctx").astype(jnp.int32)
    places = jnp.arange(N, dtype=jnp.int32)
    first = jnp.sum(jnp.where(places < index, owner_counts, 0))
    count = jnp.sum(jnp.where(places == index, owner_counts, 0))
    figures = jnp.stack([index, first - 2 * index, count, index])

    sent = pack(queries, key_rows, values, segment_ids, block_reach)
    mine = lax.all_to_all(sent, "ctx", 0, 0, tiled=True)
    theirs = lax.ppermute(mine, "ctx", [(i, i ^ 1) for i in range(N)])
    following = lax.ppermute(inner_rows[:BLOCK], "ctx", [(i, i - 1) for i in range(1, N)])
    tail = lax.ppermute(inner_rows[ROWS - 8 :], "ctx", [(i, i + 1) for i in range(N - 1)])
    out, bounds = attention(mine, theirs, (index % 2).reshape(1), owner_counts)
    received = lax.all_to_all(out.reshape(N, SLOTS * HALF, D_HEAD), "ctx", 0, 0, tiled=True)
    attn_owned = assemble(received)
    conv_owned = convolve(figures, bounds, inner_rows, following, tail, conv_weight, conv_bias)
    return attn_owned, conv_owned


def solution(mesh):
    rows = P(("dp", "ctx"), None)
    flat = P(("dp", "ctx"))
    return jax.shard_map(
        shards,
        mesh=mesh,
        in_specs=(rows, rows, rows, rows, P(), P(), flat, flat, P("dp")),
        out_specs=(rows, rows),
        check_vma=False,
    )
```

```python
import functools
import math

import jax
import jax.numpy as jnp
from jax import lax
from jax.experimental import pallas as pl
from jax.experimental.pallas import tpu as pltpu
from jax.sharding import PartitionSpec as P

HEADS = 16
D_HEAD = 128
WINDOW = 2048
BLOCK = 128
HALF = BLOCK // 2
KERNEL = 4
N = 32
ROWS = 256
SLOTS = 3
MSG = 3 * BLOCK + 8
TILES = N // 2
WIDTH = 10
EXP_SCALE = math.log2(math.e) / math.sqrt(D_HEAD)
MASKED = -1e30
GROUP = 4


def pack_kernel(reach_ref, seg_ref, q_ref, k_ref, v_ref, out_ref, held_ref, sems):
    width = GROUP * D_HEAD
    copies = {}
    for g in range(HEADS // GROUP):
        for n, ref in enumerate((q_ref, k_ref, v_ref)):
            columns = pl.ds(g * width, width)
            copies[g, n] = pltpu.make_async_copy(
                ref.at[:, columns], held_ref.at[n, :, columns], sems.at[g, n]
            )
            copies[g, n].start()
    seg = seg_ref[...]
    lane = lax.broadcasted_iota(jnp.int32, (8, 128), 1)
    meta = jnp.zeros((8, 128), jnp.int32)
    for v in range(3):
        count = jnp.sum((seg <= v).astype(jnp.int32))
        meta = jnp.where(lane == v, count, meta)
    for b in range(2):
        reach = reach_ref[b]
        meta = jnp.where(lane == 3 + 2 * b, reach // 16, meta)
        meta = jnp.where(lane == 4 + 2 * b, reach % 16, meta)
    meta = meta.astype(jnp.float32).astype(jnp.bfloat16)
    for g in range(HEADS // GROUP):
        for n in range(3):
            copies[g, n].wait()
            for h in range(g * GROUP, (g + 1) * GROUP):
                for c in range(2):
                    if n == 2:
                        columns = slice(h * D_HEAD, (h + 1) * D_HEAD)
                        out_ref[2 * h + c, n * BLOCK : (n + 1) * BLOCK, :] = jnp.concatenate(
                            [
                                held_ref[n, at : at + HALF, columns]
                                for at in (c * HALF, BLOCK + c * HALF)
                            ],
                            axis=0,
                        ).T
                        continue
                    for b in range(2):
                        at = b * BLOCK + c * HALF
                        out_ref[2 * h + c, n * BLOCK + b * HALF : n * BLOCK + (b + 1) * HALF, :] = held_ref[
                            n, at : at + HALF, h * D_HEAD : (h + 1) * D_HEAD
                        ]
    for e in range(N):
        out_ref[e, 3 * BLOCK :, :] = meta


def pack(q, k, v, seg, reach):
    anywhere = pl.BlockSpec(memory_space=pl.ANY)
    vmem = pl.BlockSpec(memory_space=pltpu.VMEM)
    return pl.pallas_call(
        pack_kernel,
        in_specs=[pl.BlockSpec(memory_space=pltpu.SMEM), vmem, anywhere, anywhere, anywhere],
        out_specs=vmem,
        out_shape=pltpu.VMEM((N, MSG, D_HEAD), jnp.bfloat16),
        scratch_shapes=[
            pltpu.VMEM((3, ROWS, HEADS * D_HEAD), jnp.bfloat16),
            pltpu.SemaphoreType.DMA((HEADS // GROUP, 3)),
        ],
        compiler_params=pltpu.CompilerParams(vmem_limit_bytes=8 << 20),
        name="pack",
    )(in_hbm(reach), in_hbm(seg.reshape(2, 128)), in_hbm(q), in_hbm(k), in_hbm(v))


def attend_kernel(
    core_ref, counts_ref, mine_ref, theirs_ref, out_ref, bounds_ref,
    s0_ref, s1_ref, m0_ref, m1_ref, pos0_ref, pos1_ref, slot_ref,
):
    core = core_ref[0]

    def fill(e, first):
        count = counts_ref[e]
        for j in range(SLOTS):
            slot_ref[first + j] = SLOTS * e + j
        for j in range(1, SLOTS):

            @pl.when(count <= j)
            def _(j=j):
                out_ref[SLOTS * e + j] = jnp.zeros((HALF, D_HEAD), jnp.bfloat16)

        return first + count

    lax.fori_loop(0, N, fill, jnp.int32(0))

    meta = mine_ref[:, 3 * BLOCK, :].astype(jnp.float32).astype(jnp.int32)
    totals = jnp.sum(meta, axis=0, keepdims=True)
    bounds = [totals[:, v : v + 1] for v in range(3)]
    lane1 = lax.broadcasted_iota(jnp.int32, (1, 128), 1)
    for v in range(3):
        bounds_ref[v] = jnp.sum(jnp.where(lane1 == v, totals, 0))

    for ref in (pos0_ref, pos1_ref):
        key = lax.broadcasted_iota(jnp.int32, (2 * BLOCK, 128), 0)
        pos = (key % BLOCK) // HALF * BLOCK + key % HALF + jnp.where(key < BLOCK, core, 1 - core) * HALF
        for w in range(WIDTH):
            ref[w * 256 : (w + 1) * 256, :] = pos + w * ROWS
    ones = jnp.ones((16, 2 * BLOCK), jnp.bfloat16)
    origin = (core // 2) * 8

    lane = lax.broadcasted_iota(jnp.int32, (1, 256), 1)

    def limits(i):
        part = lane // HALF
        first = i * (2 * ROWS) + part * BLOCK
        time = first + core * HALF + lane % HALF
        reach = jnp.zeros((1, 256), jnp.int32)
        for n in range(4):
            figures = mine_ref[2 * i + n // 2, 3 * BLOCK :, :].astype(jnp.float32).astype(jnp.int32)
            at = 3 + 2 * (n % 2)
            mine = figures[:1, at : at + 1] * 16 + figures[:1, at + 1 : at + 2]
            reach = jnp.where(part == n, mine, reach)
        low = jnp.maximum(time - (WINDOW - 1), first - reach)
        low = jnp.maximum(low, 0)
        for bound in bounds:
            low = jnp.maximum(low, jnp.where(bound <= time, bound, 0))
        start = (2 * i + 2 - WIDTH) * ROWS
        return time - start, low - start

    def keys_of(i, widths):
        parts = []
        for w in widths:
            held = jnp.maximum(2 * i + 2 - WIDTH + w, 0)
            parts += [mine_ref[held, BLOCK : 2 * BLOCK, :], theirs_ref[held, BLOCK : 2 * BLOCK, :]]
        return jnp.concatenate(parts, axis=0)

    def scores_of(i, q, widths):
        return lax.dot_general(
            keys_of(i, widths), q, (((1,), (1,)), ((), ())), preferred_element_type=jnp.float32
        )

    def keep(s, w, time, low, s_ref, pos_ref, top):
        pos = pos_ref[w * 256 : (w + 1) * 256, :]
        pos = jnp.concatenate([pos, pos], axis=1)
        allowed = pos >= low
        if w >= WIDTH - 2:
            allowed = allowed & (pos <= time)
        s = jnp.where(allowed, s, MASKED)
        s_ref[pl.ds(pl.multiple_of(origin + w * 256, 8), 256), :] = s
        here = jnp.max(s.reshape(ROWS // 8, 8, 256), axis=0)
        return here if top is None else jnp.maximum(top, here)

    def queries_of(i):
        return jnp.concatenate([mine_ref[2 * i, :BLOCK, :], mine_ref[2 * i + 1, :BLOCK, :]], axis=0)

    def weigh(i, w, s_ref, m, acc):
        held = jnp.maximum(2 * i + 2 - WIDTH + w, 0)
        p = jnp.exp2(s_ref[w * 256 : (w + 1) * 256, :] * EXP_SCALE - m).astype(jnp.bfloat16)
        vt = jnp.concatenate(
            [mine_ref[held, 2 * BLOCK : 3 * BLOCK, :], theirs_ref[held, 2 * BLOCK : 3 * BLOCK, :]], axis=1
        )
        vt = jnp.concatenate([vt, ones], axis=0)
        o = lax.dot_general(vt, p, (((1,), (0,)), ((), ())), preferred_element_type=jnp.float32)
        return o if acc is None else acc + o

    def finish_top(top, m_ref):
        m_ref[...] = jnp.broadcast_to(jnp.max(top, axis=0, keepdims=True) * EXP_SCALE, (8, 256))

    def both(i, s_ref, m_ref, ahead, s_next, m_next, pos_next):
        time, low = limits(ahead)
        q = queries_of(ahead)
        m = m_ref[:1, :]
        top = acc = None
        s = scores_of(ahead, q, range(WIDTH))
        for w in range(WIDTH):
            acc = weigh(i, w, s_ref, m, acc)
            top = keep(s[w * 256 : (w + 1) * 256], w, time, low, s_next, pos_next, top)
        finish_top(top, m_next)
        o = (acc[:D_HEAD, :] / acc[D_HEAD : D_HEAD + 1, :]).T.astype(jnp.bfloat16)
        for part in range(4):
            out_ref[slot_ref[4 * i + part]] = o[part * HALF : (part + 1) * HALF]

    time, low = limits(0)
    q, top = queries_of(0), None
    for w in range(WIDTH - 2, WIDTH):
        top = keep(scores_of(0, q, (w,)), w, time, low, s0_ref, pos0_ref, top)
    finish_top(top, m0_ref)
    s0_ref[: (WIDTH - 2) * 256, :] = jnp.full(((WIDTH - 2) * 256, 256), MASKED, jnp.float32)

    def step(n, carry):
        both(2 * n, s0_ref, m0_ref, 2 * n + 1, s1_ref, m1_ref, pos1_ref)
        both(2 * n + 1, s1_ref, m1_ref, jnp.minimum(2 * n + 2, TILES - 1), s0_ref, m0_ref, pos0_ref)
        return carry

    lax.fori_loop(0, TILES // 2, step, 0)


def attention(mine, theirs, core, counts):
    smem = pl.BlockSpec(memory_space=pltpu.SMEM)
    vmem = pl.BlockSpec(memory_space=pltpu.VMEM)
    return pl.pallas_call(
        attend_kernel,
        in_specs=[smem, smem, vmem, vmem],
        out_specs=(vmem, smem),
        out_shape=(
            jax.ShapeDtypeStruct((N * SLOTS, HALF, D_HEAD), jnp.bfloat16),
            jax.ShapeDtypeStruct((4,), jnp.int32),
        ),
        scratch_shapes=[
            pltpu.VMEM((256 * WIDTH, 256), jnp.float32),
            pltpu.VMEM((256 * WIDTH, 256), jnp.float32),
            pltpu.VMEM((8, 256), jnp.float32),
            pltpu.VMEM((8, 256), jnp.float32),
            pltpu.VMEM((256 * WIDTH, 128), jnp.int32),
            pltpu.VMEM((256 * WIDTH, 128), jnp.int32),
            pltpu.SMEM((2 * N + 8,), jnp.int32),
        ],
        cost_estimate=pl.CostEstimate(
            flops=10 * 10**9, bytes_accessed=8 * 2**20, transcendentals=10**7
        ),
        compiler_params=pltpu.CompilerParams(vmem_limit_bytes=24 << 20),
        name="attend",
    )(core, counts, in_vmem(mine), in_vmem(theirs))


def in_hbm(array):
    return pltpu.with_memory_space_constraint(array, pltpu.HBM)


def in_vmem(array):
    return pltpu.with_memory_space_constraint(array, pltpu.VMEM)


def gather_kernel(in_ref, out_ref):
    slot = pl.program_id(0)
    rows = pl.ds(pl.multiple_of(slot * HALF, HALF), HALF)
    for h in range(HEADS):
        for c in range(2):
            out_ref[c * HALF : (c + 1) * HALF, h * D_HEAD : (h + 1) * D_HEAD] = in_ref[2 * h + c, rows, :]


def assemble(received):
    return pl.pallas_call(
        gather_kernel,
        grid=(SLOTS,),
        in_specs=[pl.BlockSpec(memory_space=pltpu.VMEM)],
        out_specs=pl.BlockSpec((BLOCK, HEADS * D_HEAD), lambda j: (j, 0)),
        out_shape=jax.ShapeDtypeStruct((SLOTS * BLOCK, HEADS * D_HEAD), jnp.bfloat16),
        compiler_params=pltpu.CompilerParams(vmem_limit_bytes=8 << 20),
        name="assemble",
    )(in_vmem(received))


def conv_kernel(figures_ref, bounds_ref, inner_ref, next_ref, tail_ref, weight_ref, bias_ref, out_ref, ext_ref):
    index, off, count = figures_ref[0], figures_ref[1], figures_ref[2]
    ext_ref[:8, :] = tail_ref[...].astype(jnp.float32)
    ext_ref[8 : 8 + ROWS, :] = inner_ref[...].astype(jnp.float32)
    ext_ref[8 + ROWS :, :] = next_ref[...].astype(jnp.float32)
    for block in range(SLOTS):
        slot = block - off

        @pl.when((slot >= 0) & (slot < count))
        def _(block=block, slot=slot):
            time = index * ROWS + block * BLOCK + lax.broadcasted_iota(jnp.int32, (BLOCK, 1), 0)
            start = jnp.zeros_like(time)
            for v in range(3):
                start = jnp.maximum(start, jnp.where(bounds_ref[v] <= time, bounds_ref[v], 0))
            since = time - start
            at = 8 + block * BLOCK
            total = bias_ref[...] + weight_ref[0:1, :] * ext_ref[at : at + BLOCK, :]
            for j in range(1, KERNEL):
                row = jnp.where(since >= j, ext_ref[at - j : at - j + BLOCK, :], 0.0)
                total = total + weight_ref[j : j + 1, :] * row
            out_ref[pl.ds(pl.multiple_of(slot * BLOCK, BLOCK), BLOCK), :] = (
                total / (1.0 + jnp.exp(-total))
            ).astype(jnp.bfloat16)

    for slot in range(1, SLOTS):

        @pl.when(slot >= count)
        def _(slot=slot):
            out_ref[slot * BLOCK : (slot + 1) * BLOCK, :] = jnp.zeros((BLOCK, out_ref.shape[1]), jnp.bfloat16)


def convolve(figures, bounds, inner, following, tail, weight, bias):
    channels = inner.shape[1]
    width = 512
    smem = pl.BlockSpec(memory_space=pltpu.SMEM)

    def wide(rows):
        return pl.BlockSpec((rows, width), lambda g: (0, g))

    return pl.pallas_call(
        conv_kernel,
        grid=(channels // width,),
        in_specs=[smem, smem, wide(ROWS), wide(BLOCK), wide(8), wide(KERNEL), wide(1)],
        out_specs=wide(SLOTS * BLOCK),
        out_shape=jax.ShapeDtypeStruct((SLOTS * BLOCK, channels), jnp.bfloat16),
        scratch_shapes=[pltpu.VMEM((8 + ROWS + BLOCK, width), jnp.float32)],
        cost_estimate=pl.CostEstimate(
            flops=10 * 10**9, bytes_accessed=6 * 2**20, transcendentals=2 * 10**6
        ),
        compiler_params=pltpu.CompilerParams(vmem_limit_bytes=24 << 20),
        name="conv",
    )(figures, bounds, inner, following, tail, weight, bias.reshape(1, -1))


def shards(queries, key_rows, values, inner_rows, conv_weight, conv_bias, segment_ids, block_reach, owner_counts):
    index = lax.axis_index("ctx").astype(jnp.int32)
    places = jnp.arange(N, dtype=jnp.int32)
    first = jnp.sum(jnp.where(places < index, owner_counts, 0))
    count = jnp.sum(jnp.where(places == index, owner_counts, 0))
    figures = jnp.stack([index, first - 2 * index, count, index])

    sent = pack(queries, key_rows, values, segment_ids, block_reach)
    mine = lax.all_to_all(sent, "ctx", 0, 0, tiled=True)
    theirs = lax.ppermute(mine, "ctx", [(i, i ^ 1) for i in range(N)])
    following = lax.ppermute(inner_rows[:BLOCK], "ctx", [(i, i - 1) for i in range(1, N)])
    tail = lax.ppermute(inner_rows[ROWS - 8 :], "ctx", [(i, i + 1) for i in range(N - 1)])
    theirs, tail = lax.optimization_barrier((theirs, tail))
    out, bounds = attention(mine, theirs, (index % 2).reshape(1), owner_counts)
    received = lax.all_to_all(out.reshape(N, SLOTS * HALF, D_HEAD), "ctx", 0, 0, tiled=True)
    attn_owned = assemble(received)
    conv_owned = convolve(figures, bounds, inner_rows, following, tail, conv_weight, conv_bias)
    return attn_owned, conv_owned


def solution(mesh):
    rows = P(("dp", "ctx"), None)
    flat = P(("dp", "ctx"))
    return jax.shard_map(
        shards,
        mesh=mesh,
        in_specs=(rows, rows, rows, rows, P(), P(), flat, flat, P("dp")),
        out_specs=(rows, rows),
        check_vma=False,
    )
```

```python
import functools
import math

import jax
import jax.numpy as jnp
from jax import lax
from jax.experimental import pallas as pl
from jax.experimental.pallas import tpu as pltpu
from jax.sharding import PartitionSpec as P

HEADS = 16
D_HEAD = 128
WINDOW = 2048
BLOCK = 128
HALF = BLOCK // 2
KERNEL = 4
N = 32
ROWS = 256
SLOTS = 3
MSG = 3 * BLOCK + 8
TILES = N // 2
WIDTH = 10
WIDTHS = (6, 8, 10)
PIECES = 4
EXP_SCALE = math.log2(math.e) / math.sqrt(D_HEAD)
MASKED = -1e30
GROUP = 4


def pack_kernel(reach_ref, seg_ref, q_ref, k_ref, v_ref, inner_ref, out_ref, lead_ref, last_ref, held_ref, sems, row_sems):
    width = GROUP * D_HEAD
    copies = {}
    for g in range(HEADS // GROUP):
        for n, ref in enumerate((q_ref, k_ref, v_ref)):
            columns = pl.ds(g * width, width)
            copies[g, n] = pltpu.make_async_copy(
                ref.at[:, columns], held_ref.at[n, :, columns], sems.at[g, n]
            )
            copies[g, n].start()
    lead = pltpu.make_async_copy(inner_ref.at[pl.ds(0, BLOCK)], lead_ref, row_sems.at[0])
    last = pltpu.make_async_copy(inner_ref.at[pl.ds(ROWS - 8, 8)], last_ref, row_sems.at[1])
    lead.start()
    last.start()
    seg = seg_ref[...]
    lane = lax.broadcasted_iota(jnp.int32, (8, 128), 1)
    meta = jnp.zeros((8, 128), jnp.int32)
    for v in range(3):
        count = jnp.sum((seg <= v).astype(jnp.int32))
        meta = jnp.where(lane == v, count, meta)
    for b in range(2):
        reach = reach_ref[b]
        meta = jnp.where(lane == 3 + 2 * b, reach // 16, meta)
        meta = jnp.where(lane == 4 + 2 * b, reach % 16, meta)
    meta = meta.astype(jnp.float32).astype(jnp.bfloat16)
    for g in range(HEADS // GROUP):
        for n in range(3):
            copies[g, n].wait()
            for h in range(g * GROUP, (g + 1) * GROUP):
                for c in range(2):
                    if n == 2:
                        columns = slice(h * D_HEAD, (h + 1) * D_HEAD)
                        out_ref[2 * h + c, n * BLOCK : (n + 1) * BLOCK, :] = jnp.concatenate(
                            [
                                held_ref[n, at : at + HALF, columns]
                                for at in (c * HALF, BLOCK + c * HALF)
                            ],
                            axis=0,
                        ).T
                        continue
                    for b in range(2):
                        at = b * BLOCK + c * HALF
                        out_ref[2 * h + c, n * BLOCK + b * HALF : n * BLOCK + (b + 1) * HALF, :] = held_ref[
                            n, at : at + HALF, h * D_HEAD : (h + 1) * D_HEAD
                        ]
    for e in range(N):
        out_ref[e, 3 * BLOCK :, :] = meta
    lead.wait()
    last.wait()


def pack(q, k, v, seg, reach, inner):
    anywhere = pl.BlockSpec(memory_space=pl.ANY)
    vmem = pl.BlockSpec(memory_space=pltpu.VMEM)
    return pl.pallas_call(
        pack_kernel,
        in_specs=[pl.BlockSpec(memory_space=pltpu.SMEM), vmem, anywhere, anywhere, anywhere, anywhere],
        out_specs=(vmem, vmem, vmem),
        out_shape=(
            pltpu.VMEM((N, MSG, D_HEAD), jnp.bfloat16),
            pltpu.VMEM((BLOCK, inner.shape[1]), jnp.bfloat16),
            pltpu.VMEM((8, inner.shape[1]), jnp.bfloat16),
        ),
        scratch_shapes=[
            pltpu.VMEM((3, ROWS, HEADS * D_HEAD), jnp.bfloat16),
            pltpu.SemaphoreType.DMA((HEADS // GROUP, 3)),
            pltpu.SemaphoreType.DMA((2,)),
        ],
        compiler_params=pltpu.CompilerParams(vmem_limit_bytes=8 << 20),
        name="pack",
    )(in_hbm(reach), in_hbm(seg.reshape(2, 128)), in_hbm(q), in_hbm(k), in_hbm(v), in_hbm(inner))


def attend_kernel(
    core_ref, counts_ref, mine_ref, other_ref, out_ref, bounds_ref, theirs_ref, sems, need_ref,
    s0_ref, s1_ref, m0_ref, m1_ref, pos0_ref, pos1_ref, slot_ref,
):
    core = core_ref[0]
    size = N // PIECES
    pieces = [
        pltpu.make_async_copy(
            other_ref.at[pl.ds(p * size, size)], theirs_ref.at[pl.ds(p * size, size)], sems.at[p]
        )
        for p in range(PIECES)
    ]
    for piece in pieces:
        piece.start()

    def fill(e, first):
        count = counts_ref[e]
        for j in range(SLOTS):
            slot_ref[first + j] = SLOTS * e + j
        for j in range(1, SLOTS):

            @pl.when(count <= j)
            def _(j=j):
                out_ref[SLOTS * e + j] = jnp.zeros((HALF, D_HEAD), jnp.bfloat16)

        return first + count

    lax.fori_loop(0, N, fill, jnp.int32(0))

    meta = mine_ref[:, 3 * BLOCK, :].astype(jnp.float32).astype(jnp.int32)
    totals = jnp.sum(meta, axis=0, keepdims=True)
    bounds = [totals[:, v : v + 1] for v in range(3)]
    lane1 = lax.broadcasted_iota(jnp.int32, (1, 128), 1)
    for v in range(3):
        bounds_ref[v] = jnp.sum(jnp.where(lane1 == v, totals, 0))

    def lowest(first, reach):
        low = jnp.maximum(jnp.maximum(first - (WINDOW - 1), first - reach), 0)
        for bound in bounds:
            low = jnp.maximum(low, jnp.where(bound <= first, bound, 0))
        return low

    source = lax.broadcasted_iota(jnp.int32, (N, 1), 0)
    least = [
        lowest(source * ROWS + b * BLOCK, meta[:, 3 + 2 * b : 4 + 2 * b] * 16 + meta[:, 4 + 2 * b : 5 + 2 * b])
        for b in range(2)
    ]
    least = jnp.minimum(least[0], least[1])
    for i in range(TILES):
        need_ref[i] = 2 * i + 2 - jnp.min(jnp.where(source // 2 == i, least, N * ROWS)) // ROWS
    need_ref[TILES] = 0

    for ref in (pos0_ref, pos1_ref):
        key = lax.broadcasted_iota(jnp.int32, (2 * BLOCK, 128), 0)
        pos = (key % BLOCK) // HALF * BLOCK + key % HALF + jnp.where(key < BLOCK, core, 1 - core) * HALF
        for w in range(WIDTH):
            ref[w * 256 : (w + 1) * 256, :] = pos + w * ROWS
    ones = jnp.ones((16, 2 * BLOCK), jnp.bfloat16)
    origin = (core // 2) * 8

    lane = lax.broadcasted_iota(jnp.int32, (1, 256), 1)

    def limits(i):
        part = lane // HALF
        first = i * (2 * ROWS) + part * BLOCK
        time = first + core * HALF + lane % HALF
        reach = jnp.zeros((1, 256), jnp.int32)
        for n in range(4):
            figures = mine_ref[2 * i + n // 2, 3 * BLOCK :, :].astype(jnp.float32).astype(jnp.int32)
            at = 3 + 2 * (n % 2)
            mine = figures[:1, at : at + 1] * 16 + figures[:1, at + 1 : at + 2]
            reach = jnp.where(part == n, mine, reach)
        low = jnp.maximum(time - (WINDOW - 1), first - reach)
        low = jnp.maximum(low, 0)
        for bound in bounds:
            low = jnp.maximum(low, jnp.where(bound <= time, bound, 0))
        start = (2 * i + 2 - WIDTH) * ROWS
        return time - start, low - start

    def keys_of(i, widths):
        parts = []
        for w in widths:
            held = jnp.maximum(2 * i + 2 - WIDTH + w, 0)
            parts += [mine_ref[held, BLOCK : 2 * BLOCK, :], theirs_ref[held, BLOCK : 2 * BLOCK, :]]
        return jnp.concatenate(parts, axis=0)

    def scores_of(i, q, widths):
        return lax.dot_general(
            keys_of(i, widths), q, (((1,), (1,)), ((), ())), preferred_element_type=jnp.float32
        )

    def keep(s, w, time, low, s_ref, pos_ref, top):
        pos = pos_ref[w * 256 : (w + 1) * 256, :]
        pos = jnp.concatenate([pos, pos], axis=1)
        allowed = pos >= low
        if w >= WIDTH - 2:
            allowed = allowed & (pos <= time)
        s = jnp.where(allowed, s, MASKED)
        s_ref[pl.ds(pl.multiple_of(origin + w * 256, 8), 256), :] = s
        here = jnp.max(s.reshape(ROWS // 8, 8, 256), axis=0)
        return here if top is None else jnp.maximum(top, here)

    def queries_of(i):
        return jnp.concatenate([mine_ref[2 * i, :BLOCK, :], mine_ref[2 * i + 1, :BLOCK, :]], axis=0)

    def weigh(i, w, s_ref, m, acc):
        held = jnp.maximum(2 * i + 2 - WIDTH + w, 0)
        p = jnp.exp2(s_ref[w * 256 : (w + 1) * 256, :] * EXP_SCALE - m).astype(jnp.bfloat16)
        vt = jnp.concatenate(
            [mine_ref[held, 2 * BLOCK : 3 * BLOCK, :], theirs_ref[held, 2 * BLOCK : 3 * BLOCK, :]], axis=1
        )
        vt = jnp.concatenate([vt, ones], axis=0)
        o = lax.dot_general(vt, p, (((1,), (0,)), ((), ())), preferred_element_type=jnp.float32)
        return o if acc is None else acc + o

    def finish_top(top, m_ref):
        m_ref[...] = jnp.broadcast_to(jnp.max(top, axis=0, keepdims=True) * EXP_SCALE, (8, 256))

    def both(i, s_ref, m_ref, ahead, s_next, m_next, pos_next, width):
        time, low = limits(ahead)
        q = queries_of(ahead)
        m = m_ref[:1, :]
        top = acc = None
        skip = WIDTH - width
        s = scores_of(ahead, q, range(skip, WIDTH))
        for w in range(skip, WIDTH):
            acc = weigh(i, w, s_ref, m, acc)
            top = keep(s[(w - skip) * 256 : (w - skip + 1) * 256], w, time, low, s_next, pos_next, top)
        finish_top(top, m_next)
        o = (acc[:D_HEAD, :] / acc[D_HEAD : D_HEAD + 1, :]).T.astype(jnp.bfloat16)
        for part in range(4):
            out_ref[slot_ref[4 * i + part]] = o[part * HALF : (part + 1) * HALF]

    pieces[0].wait()
    time, low = limits(0)
    q, top = queries_of(0), None
    for w in range(WIDTH - 2, WIDTH):
        top = keep(scores_of(0, q, (w,)), w, time, low, s0_ref, pos0_ref, top)
    finish_top(top, m0_ref)

    def blank(w, carry):
        s0_ref[pl.ds(pl.multiple_of(w * 256, 256), 256), :] = jnp.full((256, 256), MASKED, jnp.float32)
        return carry

    lax.fori_loop(0, WIDTH - 2, blank, 0)

    def most(n):
        return jnp.maximum(jnp.maximum(need_ref[2 * n], need_ref[2 * n + 1]), need_ref[2 * n + 2])

    def step(n, need):
        for p in range(1, PIECES):
            @pl.when(n == (p * size - 5 + 3) // 4)
            def _(p=p):
                pieces[p].wait()

        below = 0
        for width in WIDTHS:

            @pl.when((need > below) & (need <= width))
            def _(width=width):
                both(2 * n, s0_ref, m0_ref, 2 * n + 1, s1_ref, m1_ref, pos1_ref, width)
                both(2 * n + 1, s1_ref, m1_ref, jnp.minimum(2 * n + 2, TILES - 1), s0_ref, m0_ref, pos0_ref, width)

            below = width
        later = most(jnp.minimum(n + 1, TILES // 2 - 1))
        for narrow, wide in zip(WIDTHS[:-1], WIDTHS[1:]):

            @pl.when((need <= narrow) & (later > narrow))
            def _(narrow=narrow, wide=wide):
                lax.fori_loop(WIDTH - wide, WIDTH - narrow, blank, 0)

        return later

    lax.fori_loop(0, TILES // 2, step, most(0))


def attention(mine, theirs, core, counts):
    smem = pl.BlockSpec(memory_space=pltpu.SMEM)
    vmem = pl.BlockSpec(memory_space=pltpu.VMEM)
    return pl.pallas_call(
        attend_kernel,
        in_specs=[smem, smem, vmem, pl.BlockSpec(memory_space=pl.ANY)],
        out_specs=(vmem, smem),
        out_shape=(
            pltpu.HBM((N * SLOTS, HALF, D_HEAD), jnp.bfloat16),
            jax.ShapeDtypeStruct((4,), jnp.int32),
        ),
        scratch_shapes=[
            pltpu.VMEM((N, MSG, D_HEAD), jnp.bfloat16),
            pltpu.SemaphoreType.DMA((PIECES,)),
            pltpu.SMEM((TILES + 1,), jnp.int32),
            pltpu.VMEM((256 * WIDTH, 256), jnp.float32),
            pltpu.VMEM((256 * WIDTH, 256), jnp.float32),
            pltpu.VMEM((8, 256), jnp.float32),
            pltpu.VMEM((8, 256), jnp.float32),
            pltpu.VMEM((256 * WIDTH, 128), jnp.int32),
            pltpu.VMEM((256 * WIDTH, 128), jnp.int32),
            pltpu.SMEM((2 * N + 8,), jnp.int32),
        ],
        cost_estimate=pl.CostEstimate(
            flops=10 * 10**9, bytes_accessed=8 * 2**20, transcendentals=10**7
        ),
        compiler_params=pltpu.CompilerParams(vmem_limit_bytes=24 << 20),
        name="attend",
    )(core, counts, in_vmem(mine), in_hbm(theirs))


def in_hbm(array):
    return pltpu.with_memory_space_constraint(array, pltpu.HBM)


def in_vmem(array):
    return pltpu.with_memory_space_constraint(array, pltpu.VMEM)


def gather_kernel(in_ref, out_ref):
    slot = pl.program_id(0)
    rows = pl.ds(pl.multiple_of(slot * HALF, HALF), HALF)
    for h in range(HEADS):
        for c in range(2):
            out_ref[c * HALF : (c + 1) * HALF, h * D_HEAD : (h + 1) * D_HEAD] = in_ref[2 * h + c, rows, :]


def assemble(received):
    return pl.pallas_call(
        gather_kernel,
        grid=(SLOTS,),
        in_specs=[pl.BlockSpec(memory_space=pltpu.VMEM)],
        out_specs=pl.BlockSpec((BLOCK, HEADS * D_HEAD), lambda j: (j, 0)),
        out_shape=jax.ShapeDtypeStruct((SLOTS * BLOCK, HEADS * D_HEAD), jnp.bfloat16),
        compiler_params=pltpu.CompilerParams(vmem_limit_bytes=8 << 20),
        name="assemble",
    )(in_vmem(received))


def conv_kernel(figures_ref, bounds_ref, inner_ref, next_ref, tail_ref, weight_ref, bias_ref, out_ref, ext_ref):
    index, off, count = figures_ref[0], figures_ref[1], figures_ref[2]
    ext_ref[:8, :] = tail_ref[...].astype(jnp.float32)
    ext_ref[8 : 8 + ROWS, :] = inner_ref[...].astype(jnp.float32)
    ext_ref[8 + ROWS :, :] = next_ref[...].astype(jnp.float32)
    for block in range(SLOTS):
        slot = block - off

        @pl.when((slot >= 0) & (slot < count))
        def _(block=block, slot=slot):
            time = index * ROWS + block * BLOCK + lax.broadcasted_iota(jnp.int32, (BLOCK, 1), 0)
            start = jnp.zeros_like(time)
            for v in range(3):
                start = jnp.maximum(start, jnp.where(bounds_ref[v] <= time, bounds_ref[v], 0))
            since = time - start
            at = 8 + block * BLOCK
            total = bias_ref[...] + weight_ref[0:1, :] * ext_ref[at : at + BLOCK, :]
            for j in range(1, KERNEL):
                row = jnp.where(since >= j, ext_ref[at - j : at - j + BLOCK, :], 0.0)
                total = total + weight_ref[j : j + 1, :] * row
            out_ref[pl.ds(pl.multiple_of(slot * BLOCK, BLOCK), BLOCK), :] = (
                total / (1.0 + jnp.exp(-total))
            ).astype(jnp.bfloat16)

    for slot in range(1, SLOTS):

        @pl.when(slot >= count)
        def _(slot=slot):
            out_ref[slot * BLOCK : (slot + 1) * BLOCK, :] = jnp.zeros((BLOCK, out_ref.shape[1]), jnp.bfloat16)


def convolve(figures, bounds, inner, following, tail, weight, bias):
    channels = inner.shape[1]
    width = 512
    smem = pl.BlockSpec(memory_space=pltpu.SMEM)

    def wide(rows):
        return pl.BlockSpec((rows, width), lambda g: (0, g))

    return pl.pallas_call(
        conv_kernel,
        grid=(channels // width,),
        in_specs=[smem, smem, wide(ROWS), wide(BLOCK), wide(8), wide(KERNEL), wide(1)],
        out_specs=wide(SLOTS * BLOCK),
        out_shape=jax.ShapeDtypeStruct((SLOTS * BLOCK, channels), jnp.bfloat16),
        scratch_shapes=[pltpu.VMEM((8 + ROWS + BLOCK, width), jnp.float32)],
        cost_estimate=pl.CostEstimate(
            flops=10 * 10**9, bytes_accessed=6 * 2**20, transcendentals=2 * 10**6
        ),
        compiler_params=pltpu.CompilerParams(vmem_limit_bytes=24 << 20),
        name="conv",
    )(figures, bounds, inner, following, tail, weight, bias.reshape(1, -1))


def shards(queries, key_rows, values, inner_rows, conv_weight, conv_bias, segment_ids, block_reach, owner_counts):
    index = lax.axis_index("ctx").astype(jnp.int32)
    places = jnp.arange(N, dtype=jnp.int32)
    first = jnp.sum(jnp.where(places < index, owner_counts, 0))
    count = jnp.sum(jnp.where(places == index, owner_counts, 0))
    figures = jnp.stack([index, first - 2 * index, count, index])

    sent, lead, last = pack(queries, key_rows, values, segment_ids, block_reach, inner_rows)
    mine = lax.all_to_all(sent, "ctx", 0, 0, tiled=True)
    mine, lead, last = lax.optimization_barrier((mine, lead, last))
    theirs = lax.ppermute(mine, "ctx", [(i, i ^ 1) for i in range(N)])
    following = lax.ppermute(lead, "ctx", [(i, i - 1) for i in range(1, N)])
    tail = lax.ppermute(last, "ctx", [(i, i + 1) for i in range(N - 1)])
    theirs, tail = lax.optimization_barrier((theirs, tail))
    out, bounds = attention(mine, theirs, (index % 2).reshape(1), owner_counts)
    received = lax.all_to_all(out.reshape(N, SLOTS * HALF, D_HEAD), "ctx", 0, 0, tiled=True)
    attn_owned = assemble(received)
    conv_owned = convolve(figures, bounds, inner_rows, following, tail, conv_weight, conv_bias)
    return attn_owned, conv_owned


def solution(mesh):
    rows = P(("dp", "ctx"), None)
    flat = P(("dp", "ctx"))
    return jax.shard_map(
        shards,
        mesh=mesh,
        in_specs=(rows, rows, rows, rows, P(), P(), flat, flat, P("dp")),
        out_specs=(rows, rows),
        check_vma=False,
    )
```

```python
import functools
import math

import jax
import jax.numpy as jnp
from jax import lax
from jax.experimental import pallas as pl
from jax.experimental.pallas import tpu as pltpu
from jax.sharding import PartitionSpec as P

HEADS = 16
D_HEAD = 128
WINDOW = 2048
BLOCK = 128
HALF = BLOCK // 2
KERNEL = 4
N = 32
ROWS = 256
SLOTS = 3
MSG = 3 * BLOCK + 8
TILES = N // 2
WIDTH = 10
WIDTHS = (6, 8, 10)
PIECES = 4
EXP_SCALE = math.log2(math.e) / math.sqrt(D_HEAD)
MASKED = -1e30
GROUP = 4


def pack_kernel(reach_ref, seg_ref, q_ref, k_ref, v_ref, inner_ref, out_ref, lead_ref, last_ref, held_ref, sems, row_sems):
    width = GROUP * D_HEAD
    copies = {}
    for g in range(HEADS // GROUP):
        for n, ref in enumerate((q_ref, k_ref, v_ref)):
            columns = pl.ds(g * width, width)
            copies[g, n] = pltpu.make_async_copy(
                ref.at[:, columns], held_ref.at[n, :, columns], sems.at[g, n]
            )
            if g < 2:
                copies[g, n].start()
    lead = pltpu.make_async_copy(inner_ref.at[pl.ds(0, BLOCK)], lead_ref, row_sems.at[0])
    last = pltpu.make_async_copy(inner_ref.at[pl.ds(ROWS - 8, 8)], last_ref, row_sems.at[1])
    seg = seg_ref[...]
    lane = lax.broadcasted_iota(jnp.int32, (8, 128), 1)
    meta = jnp.zeros((8, 128), jnp.int32)
    for v in range(3):
        count = jnp.sum((seg <= v).astype(jnp.int32))
        meta = jnp.where(lane == v, count, meta)
    for b in range(2):
        reach = reach_ref[b]
        meta = jnp.where(lane == 3 + 2 * b, reach // 16, meta)
        meta = jnp.where(lane == 4 + 2 * b, reach % 16, meta)
    meta = meta.astype(jnp.float32).astype(jnp.bfloat16)
    for g in range(HEADS // GROUP):
        for n in range(3):
            copies[g, n].wait()
            if (g + 2, n) in copies:
                copies[g + 2, n].start()
            elif g + 2 == HEADS // GROUP and n == 2:
                lead.start()
                last.start()
            for h in range(g * GROUP, (g + 1) * GROUP):
                for c in range(2):
                    if n == 2:
                        columns = slice(h * D_HEAD, (h + 1) * D_HEAD)
                        out_ref[2 * h + c, n * BLOCK : (n + 1) * BLOCK, :] = jnp.concatenate(
                            [
                                held_ref[n, at : at + HALF, columns]
                                for at in (c * HALF, BLOCK + c * HALF)
                            ],
                            axis=0,
                        ).T
                        continue
                    for b in range(2):
                        at = b * BLOCK + c * HALF
                        out_ref[2 * h + c, n * BLOCK + b * HALF : n * BLOCK + (b + 1) * HALF, :] = held_ref[
                            n, at : at + HALF, h * D_HEAD : (h + 1) * D_HEAD
                        ]
    for e in range(N):
        out_ref[e, 3 * BLOCK :, :] = meta
    lead.wait()
    last.wait()


def pack(q, k, v, seg, reach, inner):
    anywhere = pl.BlockSpec(memory_space=pl.ANY)
    vmem = pl.BlockSpec(memory_space=pltpu.VMEM)
    return pl.pallas_call(
        pack_kernel,
        in_specs=[pl.BlockSpec(memory_space=pltpu.SMEM), vmem, anywhere, anywhere, anywhere, anywhere],
        out_specs=(vmem, vmem, vmem),
        out_shape=(
            pltpu.VMEM((N, MSG, D_HEAD), jnp.bfloat16),
            pltpu.VMEM((BLOCK, inner.shape[1]), jnp.bfloat16),
            pltpu.VMEM((8, inner.shape[1]), jnp.bfloat16),
        ),
        scratch_shapes=[
            pltpu.VMEM((3, ROWS, HEADS * D_HEAD), jnp.bfloat16),
            pltpu.SemaphoreType.DMA((HEADS // GROUP, 3)),
            pltpu.SemaphoreType.DMA((2,)),
        ],
        compiler_params=pltpu.CompilerParams(vmem_limit_bytes=8 << 20),
        name="pack",
    )(in_hbm(reach), in_hbm(seg.reshape(2, 128)), in_hbm(q), in_hbm(k), in_hbm(v), in_hbm(inner))


def attend_kernel(
    core_ref, counts_ref, mine_ref, other_ref, out_ref, bounds_ref, theirs_ref, sems, need_ref,
    s0_ref, s1_ref, m0_ref, m1_ref, pos0_ref, pos1_ref, slot_ref,
):
    core = core_ref[0]
    size = N // PIECES
    pieces = [
        pltpu.make_async_copy(
            other_ref.at[pl.ds(p * size, size)], theirs_ref.at[pl.ds(p * size, size)], sems.at[p]
        )
        for p in range(PIECES)
    ]
    for piece in pieces:
        piece.start()

    def fill(e, first):
        count = counts_ref[e]
        for j in range(SLOTS):
            slot_ref[first + j] = SLOTS * e + j
        for j in range(1, SLOTS):

            @pl.when(count <= j)
            def _(j=j):
                out_ref[SLOTS * e + j] = jnp.zeros((HALF, D_HEAD), jnp.bfloat16)

        return first + count

    lax.fori_loop(0, N, fill, jnp.int32(0))

    meta = mine_ref[:, 3 * BLOCK, :].astype(jnp.float32).astype(jnp.int32)
    totals = jnp.sum(meta, axis=0, keepdims=True)
    bounds = [totals[:, v : v + 1] for v in range(3)]
    lane1 = lax.broadcasted_iota(jnp.int32, (1, 128), 1)
    for v in range(3):
        bounds_ref[v] = jnp.sum(jnp.where(lane1 == v, totals, 0))

    def lowest(first, reach):
        low = jnp.maximum(jnp.maximum(first - (WINDOW - 1), first - reach), 0)
        for bound in bounds:
            low = jnp.maximum(low, jnp.where(bound <= first, bound, 0))
        return low

    source = lax.broadcasted_iota(jnp.int32, (N, 1), 0)
    least = [
        lowest(source * ROWS + b * BLOCK, meta[:, 3 + 2 * b : 4 + 2 * b] * 16 + meta[:, 4 + 2 * b : 5 + 2 * b])
        for b in range(2)
    ]
    least = jnp.minimum(least[0], least[1])
    for i in range(TILES):
        need_ref[i] = 2 * i + 2 - jnp.min(jnp.where(source // 2 == i, least, N * ROWS)) // ROWS
    need_ref[TILES] = 0

    for ref in (pos0_ref, pos1_ref):
        key = lax.broadcasted_iota(jnp.int32, (2 * BLOCK, 128), 0)
        pos = (key % BLOCK) // HALF * BLOCK + key % HALF + jnp.where(key < BLOCK, core, 1 - core) * HALF
        for w in range(WIDTH):
            ref[w * 256 : (w + 1) * 256, :] = pos + w * ROWS
    ones = jnp.ones((16, 2 * BLOCK), jnp.bfloat16)
    origin = (core // 2) * 8

    lane = lax.broadcasted_iota(jnp.int32, (1, 256), 1)

    def limits(i):
        part = lane // HALF
        first = i * (2 * ROWS) + part * BLOCK
        time = first + core * HALF + lane % HALF
        reach = jnp.zeros((1, 256), jnp.int32)
        for n in range(4):
            figures = mine_ref[2 * i + n // 2, 3 * BLOCK :, :].astype(jnp.float32).astype(jnp.int32)
            at = 3 + 2 * (n % 2)
            mine = figures[:1, at : at + 1] * 16 + figures[:1, at + 1 : at + 2]
            reach = jnp.where(part == n, mine, reach)
        low = jnp.maximum(time - (WINDOW - 1), first - reach)
        low = jnp.maximum(low, 0)
        for bound in bounds:
            low = jnp.maximum(low, jnp.where(bound <= time, bound, 0))
        start = (2 * i + 2 - WIDTH) * ROWS
        return time - start, low - start

    def keys_of(i, widths):
        parts = []
        for w in widths:
            held = jnp.maximum(2 * i + 2 - WIDTH + w, 0)
            parts += [mine_ref[held, BLOCK : 2 * BLOCK, :], theirs_ref[held, BLOCK : 2 * BLOCK, :]]
        return jnp.concatenate(parts, axis=0)

    def scores_of(i, q, widths):
        return lax.dot_general(
            keys_of(i, widths), q, (((1,), (1,)), ((), ())), preferred_element_type=jnp.float32
        )

    def keep(s, w, time, low, s_ref, pos_ref, top):
        pos = pos_ref[w * 256 : (w + 1) * 256, :]
        pos = jnp.concatenate([pos, pos], axis=1)
        allowed = pos >= low
        if w >= WIDTH - 2:
            allowed = allowed & (pos <= time)
        s = jnp.where(allowed, s, MASKED)
        s_ref[pl.ds(pl.multiple_of(origin + w * 256, 8), 256), :] = s
        here = jnp.max(s.reshape(ROWS // 8, 8, 256), axis=0)
        return here if top is None else jnp.maximum(top, here)

    def queries_of(i):
        return jnp.concatenate([mine_ref[2 * i, :BLOCK, :], mine_ref[2 * i + 1, :BLOCK, :]], axis=0)

    def weigh(i, w, s_ref, m, acc):
        held = jnp.maximum(2 * i + 2 - WIDTH + w, 0)
        p = jnp.exp2(s_ref[w * 256 : (w + 1) * 256, :] * EXP_SCALE - m).astype(jnp.bfloat16)
        vt = jnp.concatenate(
            [mine_ref[held, 2 * BLOCK : 3 * BLOCK, :], theirs_ref[held, 2 * BLOCK : 3 * BLOCK, :]], axis=1
        )
        vt = jnp.concatenate([vt, ones], axis=0)
        o = lax.dot_general(vt, p, (((1,), (0,)), ((), ())), preferred_element_type=jnp.float32)
        return o if acc is None else acc + o

    def finish_top(top, m_ref):
        m_ref[...] = jnp.broadcast_to(jnp.max(top, axis=0, keepdims=True) * EXP_SCALE, (8, 256))

    def both(i, s_ref, m_ref, ahead, s_next, m_next, pos_next, width):
        time, low = limits(ahead)
        q = queries_of(ahead)
        m = m_ref[:1, :]
        top = acc = None
        skip = WIDTH - width
        s = scores_of(ahead, q, range(skip, WIDTH))
        for w in range(skip, WIDTH):
            acc = weigh(i, w, s_ref, m, acc)
            top = keep(s[(w - skip) * 256 : (w - skip + 1) * 256], w, time, low, s_next, pos_next, top)
        finish_top(top, m_next)
        o = (acc[:D_HEAD, :] / acc[D_HEAD : D_HEAD + 1, :]).T.astype(jnp.bfloat16)
        for part in range(4):
            out_ref[slot_ref[4 * i + part]] = o[part * HALF : (part + 1) * HALF]

    pieces[0].wait()
    time, low = limits(0)
    q, top = queries_of(0), None
    for w in range(WIDTH - 2, WIDTH):
        top = keep(scores_of(0, q, (w,)), w, time, low, s0_ref, pos0_ref, top)
    finish_top(top, m0_ref)

    def blank(w, carry):
        s0_ref[pl.ds(pl.multiple_of(w * 256, 256), 256), :] = jnp.full((256, 256), MASKED, jnp.float32)
        return carry

    lax.fori_loop(0, WIDTH - 2, blank, 0)

    def most(n):
        return jnp.maximum(jnp.maximum(need_ref[2 * n], need_ref[2 * n + 1]), need_ref[2 * n + 2])

    def step(n, need):
        for p in range(1, PIECES):
            @pl.when(n == (p * size - 5 + 3) // 4)
            def _(p=p):
                pieces[p].wait()

        below = 0
        for width in WIDTHS:

            @pl.when((need > below) & (need <= width))
            def _(width=width):
                both(2 * n, s0_ref, m0_ref, 2 * n + 1, s1_ref, m1_ref, pos1_ref, width)
                both(2 * n + 1, s1_ref, m1_ref, jnp.minimum(2 * n + 2, TILES - 1), s0_ref, m0_ref, pos0_ref, width)

            below = width
        later = most(jnp.minimum(n + 1, TILES // 2 - 1))
        for narrow, wide in zip(WIDTHS[:-1], WIDTHS[1:]):

            @pl.when((need <= narrow) & (later > narrow))
            def _(narrow=narrow, wide=wide):
                lax.fori_loop(WIDTH - wide, WIDTH - narrow, blank, 0)

        return later

    lax.fori_loop(0, TILES // 2, step, most(0))


def attention(mine, theirs, core, counts):
    smem = pl.BlockSpec(memory_space=pltpu.SMEM)
    vmem = pl.BlockSpec(memory_space=pltpu.VMEM)
    return pl.pallas_call(
        attend_kernel,
        in_specs=[smem, smem, vmem, pl.BlockSpec(memory_space=pl.ANY)],
        out_specs=(vmem, smem),
        out_shape=(
            pltpu.HBM((N * SLOTS, HALF, D_HEAD), jnp.bfloat16),
            jax.ShapeDtypeStruct((4,), jnp.int32),
        ),
        scratch_shapes=[
            pltpu.VMEM((N, MSG, D_HEAD), jnp.bfloat16),
            pltpu.SemaphoreType.DMA((PIECES,)),
            pltpu.SMEM((TILES + 1,), jnp.int32),
            pltpu.VMEM((256 * WIDTH, 256), jnp.float32),
            pltpu.VMEM((256 * WIDTH, 256), jnp.float32),
            pltpu.VMEM((8, 256), jnp.float32),
            pltpu.VMEM((8, 256), jnp.float32),
            pltpu.VMEM((256 * WIDTH, 128), jnp.int32),
            pltpu.VMEM((256 * WIDTH, 128), jnp.int32),
            pltpu.SMEM((2 * N + 8,), jnp.int32),
        ],
        cost_estimate=pl.CostEstimate(
            flops=10 * 10**9, bytes_accessed=8 * 2**20, transcendentals=10**7
        ),
        compiler_params=pltpu.CompilerParams(vmem_limit_bytes=24 << 20),
        name="attend",
    )(core, counts, in_vmem(mine), in_hbm(theirs))


def in_hbm(array):
    return pltpu.with_memory_space_constraint(array, pltpu.HBM)


def in_vmem(array):
    return pltpu.with_memory_space_constraint(array, pltpu.VMEM)


def gather_kernel(in_ref, out_ref, held_ref, sems):
    copies = []
    for slot in range(SLOTS):
        for h in range(HEADS):
            for c in range(2):
                held_ref[
                    slot * BLOCK + c * HALF : slot * BLOCK + (c + 1) * HALF, h * D_HEAD : (h + 1) * D_HEAD
                ] = in_ref[2 * h + c, slot * HALF : (slot + 1) * HALF, :]
        rows = pl.ds(slot * BLOCK, BLOCK)
        copies.append(pltpu.make_async_copy(held_ref.at[rows], out_ref.at[rows], sems.at[slot]))
        copies[-1].start()
    for copy in copies:
        copy.wait()


def assemble(received):
    return pl.pallas_call(
        gather_kernel,
        in_specs=[pl.BlockSpec(memory_space=pltpu.VMEM)],
        out_specs=pl.BlockSpec(memory_space=pl.ANY),
        out_shape=pltpu.HBM((SLOTS * BLOCK, HEADS * D_HEAD), jnp.bfloat16),
        scratch_shapes=[
            pltpu.VMEM((SLOTS * BLOCK, HEADS * D_HEAD), jnp.bfloat16),
            pltpu.SemaphoreType.DMA((SLOTS,)),
        ],
        compiler_params=pltpu.CompilerParams(vmem_limit_bytes=8 << 20),
        name="assemble",
    )(in_vmem(received))


def conv_kernel(figures_ref, bounds_ref, inner_ref, next_ref, tail_ref, weight_ref, bias_ref, out_ref, ext_ref):
    index, off, count = figures_ref[0], figures_ref[1], figures_ref[2]
    ext_ref[:8, :] = tail_ref[...].astype(jnp.float32)
    ext_ref[8 : 8 + ROWS, :] = inner_ref[...].astype(jnp.float32)
    ext_ref[8 + ROWS :, :] = next_ref[...].astype(jnp.float32)
    for block in range(SLOTS):
        slot = block - off

        @pl.when((slot >= 0) & (slot < count))
        def _(block=block, slot=slot):
            time = index * ROWS + block * BLOCK + lax.broadcasted_iota(jnp.int32, (BLOCK, 1), 0)
            start = jnp.zeros_like(time)
            for v in range(3):
                start = jnp.maximum(start, jnp.where(bounds_ref[v] <= time, bounds_ref[v], 0))
            since = time - start
            at = 8 + block * BLOCK
            total = bias_ref[...] + weight_ref[0:1, :] * ext_ref[at : at + BLOCK, :]
            for j in range(1, KERNEL):
                row = jnp.where(since >= j, ext_ref[at - j : at - j + BLOCK, :], 0.0)
                total = total + weight_ref[j : j + 1, :] * row
            out_ref[pl.ds(pl.multiple_of(slot * BLOCK, BLOCK), BLOCK), :] = (
                total / (1.0 + jnp.exp(-total))
            ).astype(jnp.bfloat16)

    for slot in range(1, SLOTS):

        @pl.when(slot >= count)
        def _(slot=slot):
            out_ref[slot * BLOCK : (slot + 1) * BLOCK, :] = jnp.zeros((BLOCK, out_ref.shape[1]), jnp.bfloat16)


def convolve(figures, bounds, inner, following, tail, weight, bias):
    channels = inner.shape[1]
    width = 512
    smem = pl.BlockSpec(memory_space=pltpu.SMEM)

    def wide(rows):
        return pl.BlockSpec((rows, width), lambda g: (0, g))

    return pl.pallas_call(
        conv_kernel,
        grid=(channels // width,),
        in_specs=[smem, smem, wide(ROWS), wide(BLOCK), wide(8), wide(KERNEL), wide(1)],
        out_specs=wide(SLOTS * BLOCK),
        out_shape=jax.ShapeDtypeStruct((SLOTS * BLOCK, channels), jnp.bfloat16),
        scratch_shapes=[pltpu.VMEM((8 + ROWS + BLOCK, width), jnp.float32)],
        cost_estimate=pl.CostEstimate(
            flops=10 * 10**9, bytes_accessed=6 * 2**20, transcendentals=2 * 10**6
        ),
        compiler_params=pltpu.CompilerParams(vmem_limit_bytes=24 << 20),
        name="conv",
    )(figures, bounds, inner, following, tail, weight, bias.reshape(1, -1))


def shards(queries, key_rows, values, inner_rows, conv_weight, conv_bias, segment_ids, block_reach, owner_counts):
    index = lax.axis_index("ctx").astype(jnp.int32)
    places = jnp.arange(N, dtype=jnp.int32)
    first = jnp.sum(jnp.where(places < index, owner_counts, 0))
    count = jnp.sum(jnp.where(places == index, owner_counts, 0))
    figures = jnp.stack([index, first - 2 * index, count, index])

    sent, lead, last = pack(queries, key_rows, values, segment_ids, block_reach, inner_rows)
    mine = lax.all_to_all(sent, "ctx", 0, 0, tiled=True)
    mine, lead, last = lax.optimization_barrier((mine, lead, last))
    theirs = lax.ppermute(mine, "ctx", [(i, i ^ 1) for i in range(N)])
    following = lax.ppermute(lead, "ctx", [(i, i - 1) for i in range(1, N)])
    tail = lax.ppermute(last, "ctx", [(i, i + 1) for i in range(N - 1)])
    theirs, tail = lax.optimization_barrier((theirs, tail))
    out, bounds = attention(mine, theirs, (index % 2).reshape(1), owner_counts)
    received = lax.all_to_all(out.reshape(N, SLOTS * HALF, D_HEAD), "ctx", 0, 0, tiled=True)
    attn_owned = assemble(received)
    conv_owned = convolve(figures, bounds, inner_rows, following, tail, conv_weight, conv_bias)
    return attn_owned, conv_owned


def solution(mesh):
    rows = P(("dp", "ctx"), None)
    flat = P(("dp", "ctx"))
    return jax.shard_map(
        shards,
        mesh=mesh,
        in_specs=(rows, rows, rows, rows, P(), P(), flat, flat, P("dp")),
        out_specs=(rows, rows),
        check_vma=False,
    )
```

```python
import math

import jax
import jax.numpy as jnp
from jax import lax
from jax.experimental import pallas as pl
from jax.experimental.pallas import tpu as pltpu
from jax.sharding import PartitionSpec as P


HEADS = 16
D_HEAD = 128
WINDOW = 2048
BLOCK = 128
HALF = BLOCK // 2
KERNEL = 4
N = 32
ROWS = 256
SLOTS = 3
MSG = 3 * BLOCK + 8
TILES = N // 2
WIDTH = 10
WIDTHS = (6, 8, 10)
PIECES = 4
EXP_SCALE = math.log2(math.e) / math.sqrt(D_HEAD)
MASKED = -1e30
GROUP = 4


def pack_kernel(reach_ref, seg_ref, q_ref, k_ref, v_ref, inner_ref, out_ref, lead_ref, last_ref, held_ref, sems, row_sems):
    width = GROUP * D_HEAD
    copies = {}
    for g in range(HEADS // GROUP):
        for n, ref in enumerate((q_ref, k_ref, v_ref)):
            columns = pl.ds(g * width, width)
            copies[g, n] = pltpu.make_async_copy(
                ref.at[:, columns], held_ref.at[n, :, columns], sems.at[g, n]
            )
            copies[g, n].start()
    lead = pltpu.make_async_copy(inner_ref.at[pl.ds(0, BLOCK)], lead_ref, row_sems.at[0])
    last = pltpu.make_async_copy(inner_ref.at[pl.ds(ROWS - 8, 8)], last_ref, row_sems.at[1])
    lead.start()
    last.start()
    seg = seg_ref[...]
    lane = lax.broadcasted_iota(jnp.int32, (8, 128), 1)
    meta = jnp.zeros((8, 128), jnp.int32)
    for v in range(3):
        count = jnp.sum((seg <= v).astype(jnp.int32))
        meta = jnp.where(lane == v, count, meta)
    for b in range(2):
        reach = reach_ref[b]
        meta = jnp.where(lane == 3 + 2 * b, reach // 16, meta)
        meta = jnp.where(lane == 4 + 2 * b, reach % 16, meta)
    meta = meta.astype(jnp.float32).astype(jnp.bfloat16)
    for g in range(HEADS // GROUP):
        for n in range(3):
            copies[g, n].wait()
            for h in range(g * GROUP, (g + 1) * GROUP):
                for c in range(2):
                    if n == 2:
                        columns = slice(h * D_HEAD, (h + 1) * D_HEAD)
                        out_ref[2 * h + c, n * BLOCK : (n + 1) * BLOCK, :] = jnp.concatenate(
                            [
                                held_ref[n, at : at + HALF, columns]
                                for at in (c * HALF, BLOCK + c * HALF)
                            ],
                            axis=0,
                        ).T
                        continue
                    for b in range(2):
                        at = b * BLOCK + c * HALF
                        out_ref[2 * h + c, n * BLOCK + b * HALF : n * BLOCK + (b + 1) * HALF, :] = held_ref[
                            n, at : at + HALF, h * D_HEAD : (h + 1) * D_HEAD
                        ]
    for e in range(N):
        out_ref[e, 3 * BLOCK :, :] = meta
    lead.wait()
    last.wait()


def pack(q, k, v, seg, reach, inner):
    anywhere = pl.BlockSpec(memory_space=pl.ANY)
    vmem = pl.BlockSpec(memory_space=pltpu.VMEM)
    return pl.pallas_call(
        pack_kernel,
        in_specs=[pl.BlockSpec(memory_space=pltpu.SMEM), vmem, anywhere, anywhere, anywhere, anywhere],
        out_specs=(vmem, vmem, vmem),
        out_shape=(
            pltpu.VMEM((N, MSG, D_HEAD), jnp.bfloat16),
            pltpu.VMEM((BLOCK, inner.shape[1]), jnp.bfloat16),
            pltpu.VMEM((8, inner.shape[1]), jnp.bfloat16),
        ),
        scratch_shapes=[
            pltpu.VMEM((3, ROWS, HEADS * D_HEAD), jnp.bfloat16),
            pltpu.SemaphoreType.DMA((HEADS // GROUP, 3)),
            pltpu.SemaphoreType.DMA((2,)),
        ],
        compiler_params=pltpu.CompilerParams(vmem_limit_bytes=8 << 20),
        name="pack",
    )(in_hbm(reach), in_hbm(seg.reshape(2, 128)), in_hbm(q), in_hbm(k), in_hbm(v), in_hbm(inner))


def attend_kernel(
    core_ref, counts_ref, mine_ref, other_ref, out_ref, bounds_ref, theirs_ref, sems, need_ref,
    s0_ref, s1_ref, m0_ref, m1_ref, pos0_ref, pos1_ref, slot_ref,
):
    core = core_ref[0]
    size = N // PIECES
    pieces = [
        pltpu.make_async_copy(
            other_ref.at[pl.ds(p * size, size)], theirs_ref.at[pl.ds(p * size, size)], sems.at[p]
        )
        for p in range(PIECES)
    ]
    for piece in pieces:
        piece.start()

    def fill(e, first):
        count = counts_ref[e]
        for j in range(SLOTS):
            slot_ref[first + j] = SLOTS * e + j
        for j in range(1, SLOTS):

            @pl.when(count <= j)
            def _(j=j):
                out_ref[SLOTS * e + j] = jnp.zeros((HALF, D_HEAD), jnp.bfloat16)

        return first + count

    lax.fori_loop(0, N, fill, jnp.int32(0))

    meta = mine_ref[:, 3 * BLOCK, :].astype(jnp.float32).astype(jnp.int32)
    totals = jnp.sum(meta, axis=0, keepdims=True)
    bounds = [totals[:, v : v + 1] for v in range(3)]
    lane1 = lax.broadcasted_iota(jnp.int32, (1, 128), 1)
    for v in range(3):
        bounds_ref[v] = jnp.sum(jnp.where(lane1 == v, totals, 0))

    def lowest(first, reach):
        low = jnp.maximum(jnp.maximum(first - (WINDOW - 1), first - reach), 0)
        for bound in bounds:
            low = jnp.maximum(low, jnp.where(bound <= first, bound, 0))
        return low

    source = lax.broadcasted_iota(jnp.int32, (N, 1), 0)
    least = [
        lowest(source * ROWS + b * BLOCK, meta[:, 3 + 2 * b : 4 + 2 * b] * 16 + meta[:, 4 + 2 * b : 5 + 2 * b])
        for b in range(2)
    ]
    least = jnp.minimum(least[0], least[1])
    for i in range(TILES):
        need_ref[i] = 2 * i + 2 - jnp.min(jnp.where(source // 2 == i, least, N * ROWS)) // ROWS
    need_ref[TILES] = 0

    for ref in (pos0_ref, pos1_ref):
        key = lax.broadcasted_iota(jnp.int32, (2 * BLOCK, 128), 0)
        pos = (key % BLOCK) // HALF * BLOCK + key % HALF + jnp.where(key < BLOCK, core, 1 - core) * HALF
        for w in range(WIDTH):
            ref[w * 256 : (w + 1) * 256, :] = pos + w * ROWS
    ones = jnp.ones((16, 2 * BLOCK), jnp.bfloat16)
    origin = (core // 2) * 8

    lane = lax.broadcasted_iota(jnp.int32, (1, 256), 1)

    def limits(i):
        part = lane // HALF
        first = i * (2 * ROWS) + part * BLOCK
        time = first + core * HALF + lane % HALF
        reach = jnp.zeros((1, 256), jnp.int32)
        for n in range(4):
            figures = mine_ref[2 * i + n // 2, 3 * BLOCK :, :].astype(jnp.float32).astype(jnp.int32)
            at = 3 + 2 * (n % 2)
            mine = figures[:1, at : at + 1] * 16 + figures[:1, at + 1 : at + 2]
            reach = jnp.where(part == n, mine, reach)
        low = jnp.maximum(time - (WINDOW - 1), first - reach)
        low = jnp.maximum(low, 0)
        for bound in bounds:
            low = jnp.maximum(low, jnp.where(bound <= time, bound, 0))
        start = (2 * i + 2 - WIDTH) * ROWS
        return time - start, low - start

    def keys_of(i, widths):
        parts = []
        for w in widths:
            held = jnp.maximum(2 * i + 2 - WIDTH + w, 0)
            parts += [mine_ref[held, BLOCK : 2 * BLOCK, :], theirs_ref[held, BLOCK : 2 * BLOCK, :]]
        return jnp.concatenate(parts, axis=0)

    def scores_of(i, q, widths):
        return lax.dot_general(
            keys_of(i, widths), q, (((1,), (1,)), ((), ())), preferred_element_type=jnp.float32
        )

    def keep(s, w, time, low, s_ref, pos_ref, top):
        pos = pos_ref[w * 256 : (w + 1) * 256, :]
        pos = jnp.concatenate([pos, pos], axis=1)
        allowed = pos >= low
        if w >= WIDTH - 2:
            allowed = allowed & (pos <= time)
        s = jnp.where(allowed, s, MASKED)
        s_ref[pl.ds(pl.multiple_of(origin + w * 256, 8), 256), :] = s
        here = jnp.max(s.reshape(ROWS // 8, 8, 256), axis=0)
        return here if top is None else jnp.maximum(top, here)

    def queries_of(i):
        return jnp.concatenate([mine_ref[2 * i, :BLOCK, :], mine_ref[2 * i + 1, :BLOCK, :]], axis=0)

    def weigh(i, w, s_ref, m, acc):
        held = jnp.maximum(2 * i + 2 - WIDTH + w, 0)
        p = jnp.exp2(s_ref[w * 256 : (w + 1) * 256, :] * EXP_SCALE - m).astype(jnp.bfloat16)
        vt = jnp.concatenate(
            [mine_ref[held, 2 * BLOCK : 3 * BLOCK, :], theirs_ref[held, 2 * BLOCK : 3 * BLOCK, :]], axis=1
        )
        vt = jnp.concatenate([vt, ones], axis=0)
        o = lax.dot_general(vt, p, (((1,), (0,)), ((), ())), preferred_element_type=jnp.float32)
        return o if acc is None else acc + o

    def finish_top(top, m_ref):
        m_ref[...] = jnp.broadcast_to(jnp.max(top, axis=0, keepdims=True) * EXP_SCALE, (8, 256))

    def both(i, s_ref, m_ref, ahead, s_next, m_next, pos_next, width):
        time, low = limits(ahead)
        q = queries_of(ahead)
        m = m_ref[:1, :]
        top = acc = None
        skip = WIDTH - width
        s = scores_of(ahead, q, range(skip, WIDTH))
        for w in range(skip, WIDTH):
            acc = weigh(i, w, s_ref, m, acc)
            top = keep(s[(w - skip) * 256 : (w - skip + 1) * 256], w, time, low, s_next, pos_next, top)
        finish_top(top, m_next)
        o = (acc[:D_HEAD, :] / acc[D_HEAD : D_HEAD + 1, :]).T.astype(jnp.bfloat16)
        for part in range(4):
            out_ref[slot_ref[4 * i + part]] = o[part * HALF : (part + 1) * HALF]

    pieces[0].wait()
    time, low = limits(0)
    q, top = queries_of(0), None
    for w in range(WIDTH - 2, WIDTH):
        top = keep(scores_of(0, q, (w,)), w, time, low, s0_ref, pos0_ref, top)
    finish_top(top, m0_ref)

    def blank(w, carry):
        s0_ref[pl.ds(pl.multiple_of(w * 256, 256), 256), :] = jnp.full((256, 256), MASKED, jnp.float32)
        return carry

    lax.fori_loop(0, WIDTH - 2, blank, 0)

    def most(n):
        return jnp.maximum(jnp.maximum(need_ref[2 * n], need_ref[2 * n + 1]), need_ref[2 * n + 2])

    def step(n, need):
        for p in range(1, PIECES):
            @pl.when(n == (p * size - 5 + 3) // 4)
            def _(p=p):
                pieces[p].wait()

        below = 0
        for width in WIDTHS:

            @pl.when((need > below) & (need <= width))
            def _(width=width):
                both(2 * n, s0_ref, m0_ref, 2 * n + 1, s1_ref, m1_ref, pos1_ref, width)
                both(2 * n + 1, s1_ref, m1_ref, jnp.minimum(2 * n + 2, TILES - 1), s0_ref, m0_ref, pos0_ref, width)

            below = width
        later = most(jnp.minimum(n + 1, TILES // 2 - 1))
        for narrow, wide in zip(WIDTHS[:-1], WIDTHS[1:]):

            @pl.when((need <= narrow) & (later > narrow))
            def _(narrow=narrow, wide=wide):
                lax.fori_loop(WIDTH - wide, WIDTH - narrow, blank, 0)

        return later

    lax.fori_loop(0, TILES // 2, step, most(0))


def attention(mine, theirs, core, counts):
    smem = pl.BlockSpec(memory_space=pltpu.SMEM)
    vmem = pl.BlockSpec(memory_space=pltpu.VMEM)
    return pl.pallas_call(
        attend_kernel,
        in_specs=[smem, smem, vmem, pl.BlockSpec(memory_space=pl.ANY)],
        out_specs=(vmem, smem),
        out_shape=(
            pltpu.HBM((N * SLOTS, HALF, D_HEAD), jnp.bfloat16),
            jax.ShapeDtypeStruct((4,), jnp.int32),
        ),
        scratch_shapes=[
            pltpu.VMEM((N, MSG, D_HEAD), jnp.bfloat16),
            pltpu.SemaphoreType.DMA((PIECES,)),
            pltpu.SMEM((TILES + 1,), jnp.int32),
            pltpu.VMEM((256 * WIDTH, 256), jnp.float32),
            pltpu.VMEM((256 * WIDTH, 256), jnp.float32),
            pltpu.VMEM((8, 256), jnp.float32),
            pltpu.VMEM((8, 256), jnp.float32),
            pltpu.VMEM((256 * WIDTH, 128), jnp.int32),
            pltpu.VMEM((256 * WIDTH, 128), jnp.int32),
            pltpu.SMEM((2 * N + 8,), jnp.int32),
        ],
        cost_estimate=pl.CostEstimate(
            flops=10 * 10**9, bytes_accessed=8 * 2**20, transcendentals=10**7
        ),
        compiler_params=pltpu.CompilerParams(vmem_limit_bytes=24 << 20),
        name="attend",
    )(core, counts, in_vmem(mine), in_hbm(theirs))


def in_hbm(array):
    return pltpu.with_memory_space_constraint(array, pltpu.HBM)


def in_vmem(array):
    return pltpu.with_memory_space_constraint(array, pltpu.VMEM)


def gather_kernel(in_ref, out_ref, held_ref, sems):
    copies = []
    for slot in range(SLOTS):
        for h in range(HEADS):
            for c in range(2):
                held_ref[
                    slot * BLOCK + c * HALF : slot * BLOCK + (c + 1) * HALF, h * D_HEAD : (h + 1) * D_HEAD
                ] = in_ref[2 * h + c, slot * HALF : (slot + 1) * HALF, :]
        rows = pl.ds(slot * BLOCK, BLOCK)
        copies.append(pltpu.make_async_copy(held_ref.at[rows], out_ref.at[rows], sems.at[slot]))
        copies[-1].start()
    for copy in copies:
        copy.wait()


def assemble(received):
    return pl.pallas_call(
        gather_kernel,
        in_specs=[pl.BlockSpec(memory_space=pltpu.VMEM)],
        out_specs=pl.BlockSpec(memory_space=pl.ANY),
        out_shape=pltpu.HBM((SLOTS * BLOCK, HEADS * D_HEAD), jnp.bfloat16),
        scratch_shapes=[
            pltpu.VMEM((SLOTS * BLOCK, HEADS * D_HEAD), jnp.bfloat16),
            pltpu.SemaphoreType.DMA((SLOTS,)),
        ],
        compiler_params=pltpu.CompilerParams(vmem_limit_bytes=8 << 20),
        name="assemble",
    )(in_vmem(received))


def conv_kernel(figures_ref, bounds_ref, inner_ref, next_ref, tail_ref, weight_ref, bias_ref, out_ref, ext_ref):
    index, off, count = figures_ref[0], figures_ref[1], figures_ref[2]
    ext_ref[:8, :] = tail_ref[...].astype(jnp.float32)
    ext_ref[8 : 8 + ROWS, :] = inner_ref[...].astype(jnp.float32)
    ext_ref[8 + ROWS :, :] = next_ref[...].astype(jnp.float32)
    for block in range(SLOTS):
        slot = block - off

        @pl.when((slot >= 0) & (slot < count))
        def _(block=block, slot=slot):
            time = index * ROWS + block * BLOCK + lax.broadcasted_iota(jnp.int32, (BLOCK, 1), 0)
            start = jnp.zeros_like(time)
            for v in range(3):
                start = jnp.maximum(start, jnp.where(bounds_ref[v] <= time, bounds_ref[v], 0))
            since = time - start
            at = 8 + block * BLOCK
            total = bias_ref[...] + weight_ref[0:1, :] * ext_ref[at : at + BLOCK, :]
            for j in range(1, KERNEL):
                row = jnp.where(since >= j, ext_ref[at - j : at - j + BLOCK, :], 0.0)
                total = total + weight_ref[j : j + 1, :] * row
            out_ref[pl.ds(pl.multiple_of(slot * BLOCK, BLOCK), BLOCK), :] = (
                total / (1.0 + jnp.exp(-total))
            ).astype(jnp.bfloat16)

    for slot in range(1, SLOTS):

        @pl.when(slot >= count)
        def _(slot=slot):
            out_ref[slot * BLOCK : (slot + 1) * BLOCK, :] = jnp.zeros((BLOCK, out_ref.shape[1]), jnp.bfloat16)


def convolve(figures, bounds, inner, following, tail, weight, bias):
    channels = inner.shape[1]
    width = 512
    smem = pl.BlockSpec(memory_space=pltpu.SMEM)

    def wide(rows):
        return pl.BlockSpec((rows, width), lambda g: (0, g))

    return pl.pallas_call(
        conv_kernel,
        grid=(channels // width,),
        in_specs=[smem, smem, wide(ROWS), wide(BLOCK), wide(8), wide(KERNEL), wide(1)],
        out_specs=wide(SLOTS * BLOCK),
        out_shape=jax.ShapeDtypeStruct((SLOTS * BLOCK, channels), jnp.bfloat16),
        scratch_shapes=[pltpu.VMEM((8 + ROWS + BLOCK, width), jnp.float32)],
        cost_estimate=pl.CostEstimate(
            flops=10 * 10**9, bytes_accessed=6 * 2**20, transcendentals=2 * 10**6
        ),
        compiler_params=pltpu.CompilerParams(vmem_limit_bytes=24 << 20),
        name="conv",
    )(figures, bounds, inner, following, tail, weight, bias.reshape(1, -1))


def shards(queries, key_rows, values, inner_rows, conv_weight, conv_bias, segment_ids, block_reach, owner_counts):
    index = lax.axis_index("ctx").astype(jnp.int32)
    places = jnp.arange(N, dtype=jnp.int32)
    first = jnp.sum(jnp.where(places < index, owner_counts, 0))
    count = jnp.sum(jnp.where(places == index, owner_counts, 0))
    figures = jnp.stack([index, first - 2 * index, count, index])

    sent, lead, last = pack(queries, key_rows, values, segment_ids, block_reach, inner_rows)
    mine = lax.all_to_all(sent, "ctx", 0, 0, tiled=True)
    mine, lead, last = lax.optimization_barrier((mine, lead, last))
    theirs = lax.ppermute(mine, "ctx", [(i, i ^ 1) for i in range(N)])
    following = lax.ppermute(lead, "ctx", [(i, i - 1) for i in range(1, N)])
    tail = lax.ppermute(last, "ctx", [(i, i + 1) for i in range(N - 1)])
    out, bounds = attention(mine, theirs, (index % 2).reshape(1), owner_counts)
    received = lax.all_to_all(out.reshape(N, SLOTS * HALF, D_HEAD), "ctx", 0, 0, tiled=True)
    attn_owned = assemble(received)
    conv_owned = convolve(figures, bounds, inner_rows, following, tail, conv_weight, conv_bias)
    return attn_owned, conv_owned


def solution(mesh):
    rows = P(("dp", "ctx"), None)
    flat = P(("dp", "ctx"))
    return jax.shard_map(
        shards,
        mesh=mesh,
        in_specs=(rows, rows, rows, rows, P(), P(), flat, flat, P("dp")),
        out_specs=(rows, rows),
        check_vma=False,
    )
```
